256 devices in a mesh: src: 8 (over x, y_hi), rcv: 32 (over y_lo, z, core).
Axes of the slice: x: 4, y: 4 (y_hi: 2, y_lo: 2; y = y_hi * 2 + y_lo), z: 8, core: 2. Of those that a mesh axis runs over, the one named last changes fastest.
Arguments:
- wavefield: float32 [2, 16, 2048, 2048], P(None, None, 'rcv', 'src')
- surface_band: float32 [2, 2048, 1024], P(None, 'rcv'), may hold values from -0.75 to 0.75
- band_shift: int32 [32], P('rcv'), may hold values from -16 to 16
- trace_mask: int32 [2048], P('rcv'), may hold values 0 or 1
- shot_taper: float32 [5], replicated, may hold values from 0.2 to 1
Outputs:
- multiples: float32 [2, 16, 2048, 2048], P(None, None, 'rcv', 'src')
- primaries: float32 [2, 16, 2048, 2048], P(None, None, 'rcv', 'src')
The draws below stay inside these ranges and needn't reach their ends.
All inputs are finite; a program needn't handle non-finite values. No bound on the sum of `trace_mask` on one device may be relied on, other than what follows from the above.
Results may differ from the reference program's by a relative error of at most 0.0003.
Values sent between devices are 32-bit elements; how exact they have to be, the bound alone decides.
No kernel may reach another device: no remote copies, remote signals or barrier semaphores. Data moves between devices by JAX's collectives and lax.ppermute only.
A program may use at most 64 MiB of HBM per device.

```python
import jax
import jax.numpy as jnp
from jax import lax

F = 16
NS = 2048
NR = 2048
APER = 64
SHIFT = 16
BLOCK = 64
SHALF = 2


def draw_wavefield(key, part):
    base_key = jax.random.fold_in(key, 7)
    noise_key, row_key, col_key = jax.random.split(base_key, 3)
    rows = jnp.exp(jax.random.uniform(row_key, (NS,), jnp.float32, -1.15, 1.15)) * jnp.exp(1.0986 * (jnp.arange(NS, dtype=jnp.float32) / NS - 0.5))
    cols = jnp.exp(jax.random.uniform(col_key, (NR,), jnp.float32, -1.15, 1.15)) * jnp.exp(1.0986 * (jnp.arange(NR, dtype=jnp.float32) / NR - 0.5))
    noise = jax.random.normal(noise_key, (2, F, NR, NS), jnp.float32)
    return noise * cols[None, None, :, None] * rows[None, None, None, :] * 0.5


def touch_ends(array, key, least, largest):
    place = [jax.random.randint(jax.random.fold_in(key, axis), (), 0, length) for axis, length in enumerate(array.shape)]
    longest = array.shape.index(max(array.shape))
    neighbour = place[:longest] + [(place[longest] + 1) % array.shape[longest]] + place[longest + 1:]
    return array.at[tuple(place)].set(least).at[tuple(neighbour)].set(largest)


def levels(stream_key, extent, cuts, low, top_value):
    level, own = 1.0, jax.random.fold_in(stream_key, 6)
    for position, shards_of in cuts:
        heights = jnp.exp(jax.random.uniform(jax.random.fold_in(own, position), (shards_of,), jnp.float32, low / len(cuts), top_value / len(cuts)))
        level = level * jnp.repeat(heights, extent[position] // shards_of).reshape([-1 if axis == position else 1 for axis in range(len(extent))])
    return level


def gaussian(stream_key, extent, spread, limit, shards=(), kind=jnp.bfloat16):
    level = levels(stream_key, extent, shards, -0.22, 0.18) if shards else 1.0
    drawn = jax.random.normal(stream_key, extent, jnp.float32) * spread * level
    return jnp.minimum(jnp.maximum(drawn, -limit), limit).astype(kind)


def setup_inputs(seed: int = 0) -> dict:
    key_of = jax.random.split(jax.random.key(seed), 6)
    wavefield = draw_wavefield(jax.random.fold_in(key_of[5], 71), 0)
    surface_band = gaussian(key_of[1], (2, NR, F * APER), APER ** -0.5, 0.75, ((1, 32),), jnp.float32)
    band_shift = touch_ends(jax.random.randint(key_of[2], (NR // BLOCK,), -SHIFT, SHIFT + 1), jax.random.fold_in(key_of[2], 1), -SHIFT, SHIFT).astype(jnp.int32)
    trace_mask = touch_ends((jax.random.randint(key_of[3], (NR,), 0, 8) < 7).astype(jnp.int32), jax.random.fold_in(key_of[3], 1), 0, 1)
    shot_taper = jnp.clip(jax.random.uniform(key_of[4], (2 * SHALF + 1,), jnp.float32, 0.2, 1.0), 0.2, 1.0)
    return dict(wavefield=wavefield, surface_band=surface_band, band_shift=band_shift, trace_mask=trace_mask, shot_taper=shot_taper)


def band_matrix(band_piece):
    columns = band_piece.shape[3]
    taps = band_piece.shape[2]
    rows_index = jnp.arange(columns + taps - 1, dtype=jnp.int32)
    cols_index = jnp.arange(columns, dtype=jnp.int32)
    tap_index = jnp.arange(taps, dtype=jnp.int32)
    onehot = (tap_index[:, None, None] == rows_index[None, :, None] - cols_index[None, None, :]).astype(jnp.float32)
    return jnp.einsum('xftc,tjc->xfjc', band_piece, onehot, precision=lax.Precision.HIGHEST)

def complex_product(window, band):
    real_part = jnp.einsum('fjc,fjs->fcs', band[0], window[0], precision=lax.Precision.HIGHEST) - jnp.einsum('fjc,fjs->fcs', band[1], window[1], precision=lax.Precision.HIGHEST)
    imag_part = jnp.einsum('fjc,fjs->fcs', band[1], window[0], precision=lax.Precision.HIGHEST) + jnp.einsum('fjc,fjs->fcs', band[0], window[1], precision=lax.Precision.HIGHEST)
    return jnp.stack([real_part, imag_part])

def reference(wavefield, surface_band, band_shift, trace_mask, shot_taper):
    masked = wavefield * trace_mask.astype(jnp.float32)[None, None, :, None]
    halo_width = APER // 2 + SHIFT
    padded = jnp.pad(masked, ((0, 0), (0, 0), (halo_width, halo_width), (0, 0)))
    band_full = jnp.transpose(surface_band.reshape(2, NR, F, APER), (0, 2, 3, 1))

    def one_block(index):
        start = index * BLOCK + halo_width - APER // 2 + band_shift[index]
        window = lax.dynamic_slice_in_dim(padded, start.astype(jnp.int32), BLOCK + APER - 1, 2)
        band_piece = lax.dynamic_slice_in_dim(band_full, (index * BLOCK).astype(jnp.int32), BLOCK, 3)
        return complex_product(window, band_matrix(band_piece))
    stacked = lax.map(one_block, jnp.arange(NR // BLOCK, dtype=jnp.int32))
    predicted = jnp.moveaxis(stacked, 0, 2).reshape(2, F, NR, NS)
    shot_padded = jnp.pad(predicted, ((0, 0), (0, 0), (0, 0), (SHALF, SHALF)))
    multiples = jnp.zeros_like(predicted)
    for offset_row in range(2 * SHALF + 1):
        multiples = multiples + shot_taper[offset_row] * shot_padded[:, :, :, offset_row:offset_row + NS]
    data_energy = lax.optimization_barrier(jnp.sum(wavefield * wavefield, axis=(0, 2, 3)))
    pred_energy = lax.optimization_barrier(jnp.sum(multiples * multiples, axis=(0, 2, 3)))
    gain = jnp.sqrt((data_energy + 1e-06) / (pred_energy + 1e-06))
    primaries = wavefield - gain[None, :, None, None] * multiples
    return (multiples, primaries)
```

```python
import jax
import jax.numpy as jnp
from jax import lax
from jax.sharding import Mesh
from jax.sharding import PartitionSpec as P

APER = 64
SHIFT = 16
BLOCK = 64
SHALF = 2
RCV = ("rcv_0", "rcv_1", "rcv_2")
SRC = ("src_0", "src_1")
SRC_RCV = ("src_0", "src_1", "rcv_0", "rcv_1", "rcv_2")


def extended(cells, sides, width):
    for axis, dim in sides:
        count = lax.axis_size(axis)
        ends = count - 1
        head = lax.slice_in_dim(cells, 0, width, axis=dim)
        tail = lax.slice_in_dim(cells, cells.shape[dim] - width, cells.shape[dim], axis=dim)
        cells = jnp.concatenate(
            [
                lax.ppermute(tail, axis, [(i, (i + 1) % count) for i in range(ends)]),
                cells,
                lax.ppermute(head, axis, [((i + 1) % count, i) for i in range(ends)]),
            ],
            axis=dim,
        )
    return cells


def summed_everywhere(rows, axes):
    count = lax.axis_size(axes)
    spread = jnp.broadcast_to(rows[None], (count,) + rows.shape)
    return jnp.sum(lax.all_to_all(spread, axes, 0, 0, tiled=True), axis=0)


def band_matrix(band_piece):
    columns = band_piece.shape[3]
    taps = band_piece.shape[2]
    rows_index = jnp.arange(columns + taps - 1, dtype=jnp.int32)
    cols_index = jnp.arange(columns, dtype=jnp.int32)
    tap_index = jnp.arange(taps, dtype=jnp.int32)
    onehot = (
        tap_index[:, None, None] == rows_index[None, :, None] - cols_index[None, None, :]
    ).astype(jnp.float32)
    return jnp.einsum("xftc,tjc->xfjc", band_piece, onehot, precision=lax.Precision.HIGHEST)


def complex_product(window, band):
    real_part = jnp.einsum(
        "fjc,fjs->fcs", band[0], window[0], precision=lax.Precision.HIGHEST
    ) - jnp.einsum("fjc,fjs->fcs", band[1], window[1], precision=lax.Precision.HIGHEST)
    imag_part = jnp.einsum(
        "fjc,fjs->fcs", band[1], window[0], precision=lax.Precision.HIGHEST
    ) + jnp.einsum("fjc,fjs->fcs", band[0], window[1], precision=lax.Precision.HIGHEST)
    return jnp.stack([real_part, imag_part])


def receiver_products(padded, band_local, band_shift, halo_width):
    start = halo_width - APER // 2 + band_shift[0]
    window = lax.dynamic_slice_in_dim(padded, start, BLOCK + APER - 1, 2)
    outputs = complex_product(window, band_matrix(band_local))
    return outputs


def taper_rows(padded, shot_taper, shots):
    result = shot_taper[0] * padded[:, :, :, 0:shots]
    for offset_row in range(1, 2 * SHALF + 1):
        result = result + shot_taper[offset_row] * padded[:, :, :, offset_row : offset_row + shots]
    return result


def per_device(wavefield, surface_band, band_shift, trace_mask, shot_taper):
    shots = wavefield.shape[3]
    slices = wavefield.shape[1]
    receivers = wavefield.shape[2]
    band_local = jnp.transpose(surface_band.reshape(2, receivers, slices, APER), (0, 2, 3, 1))
    masked = wavefield * trace_mask.astype(jnp.float32)[None, None, :, None]
    halo_width = APER // 2 + SHIFT
    padded = extended(masked, ((RCV, 2),), halo_width)
    predicted = receiver_products(padded, band_local, band_shift, halo_width)
    shot_padded = extended(predicted, ((SRC, 3),), SHALF)
    multiples = taper_rows(shot_padded, shot_taper, shots)
    data_energy = jnp.sum(wavefield * wavefield, axis=(0, 2, 3))
    pred_energy = jnp.sum(multiples * multiples, axis=(0, 2, 3))
    partial = jnp.concatenate([data_energy, pred_energy])[None]
    partial = jnp.pad(partial, ((0, 0), (0, 128 - partial.shape[1])))
    total = summed_everywhere(partial, SRC_RCV)[0]
    data_energy, pred_energy = (total[:slices], total[slices : 2 * slices])
    gain = jnp.sqrt((data_energy + 1e-06) / (pred_energy + 1e-06))
    primaries = wavefield - gain[None, :, None, None] * multiples
    return (multiples, primaries)


def solution(mesh):
    split = Mesh(mesh.devices.reshape(4, 2, 2, 8, 2), ("src_0", "src_1", "rcv_0", "rcv_1", "rcv_2"))
    return jax.shard_map(
        per_device,
        mesh=split,
        in_specs=(P(None, None, RCV, SRC), P(None, RCV, None), P(RCV), P(RCV), P()),
        out_specs=(P(None, None, RCV, SRC), P(None, None, RCV, SRC)),
        check_vma=False,
    )
```

```python
import functools

import jax
import jax.numpy as jnp
from jax import lax
from jax.experimental import pallas as pl
from jax.experimental.pallas import tpu as pltpu
from jax.sharding import Mesh
from jax.sharding import PartitionSpec as P

APER = 64
SHIFT = 16
BLOCK = 64
SHALF = 2
HALO = APER // 2 + SHIFT
LANES = 128
RCV = ("rcv_0", "rcv_1", "rcv_2")
SRC = ("src_0", "src_1")
SRC_RCV = ("src_0", "src_1", "rcv_0", "rcv_1", "rcv_2")
F32 = jnp.float32
BF16 = jnp.bfloat16


def iota(shape, dim):
    return lax.broadcasted_iota(jnp.int32, shape, dim)


def split(x):
    high = x.astype(BF16)
    return high, (x - high.astype(F32)).astype(BF16)


def product(a, b, transposed=False):
    dims = (((1,), (1 if transposed else 0,)), ((), ()))
    dot = functools.partial(lax.dot_general, dimension_numbers=dims, preferred_element_type=F32)
    return dot(a[0], b[0]) + (dot(a[0], b[1]) + dot(a[1], b[0]))


def mask_column(mask_ref):
    row = jnp.broadcast_to(mask_ref[...].astype(F32), (BLOCK, BLOCK))
    diagonal = iota((BLOCK, BLOCK), 0) == iota((BLOCK, BLOCK), 1)
    return jnp.sum(jnp.where(diagonal, row, 0.0), axis=1, keepdims=True)


def prepare_kernel(wave_ref, mask_ref, left_ref, right_ref, first_ref, last_ref):
    mask = mask_column(mask_ref)
    shots = wave_ref.shape[3]
    picked = iota((8, shots), 0)
    picked = jnp.where(picked < SHALF, picked, picked + (shots - 8))
    select = (iota((8, shots), 1) == picked).astype(F32)
    for f in range(wave_ref.shape[1]):
        parts = []
        for x in range(2):
            masked = wave_ref[x, f] * mask
            left_ref[x, f] = masked[:HALO]
            right_ref[x, f] = masked[BLOCK - HALO :]
            parts.append(masked)
        ends = lax.dot_general(
            select,
            jnp.concatenate(parts, axis=0),
            (((1,), (1,)), ((), ())),
            precision=lax.Precision.HIGHEST,
            preferred_element_type=F32,
        )
        first_ref[:, f * LANES : (f + 1) * LANES] = ends[:SHALF]
        last_ref[:, f * LANES : (f + 1) * LANES] = ends[8 - SHALF :]


def own_kernel(shift_ref, wave_ref, mask_ref, band_ref, oh_ref, ol_ref, hh_ref, hl_ref, pred_ref, energy_ref):
    shift = shift_ref[0]
    mask = mask_column(mask_ref)
    low_half = iota((BLOCK, LANES), 1) < APER
    from_left = iota((2 * BLOCK, LANES), 0) % BLOCK + shift < APER // 2
    for f in range(wave_ref.shape[1]):
        at = (f // 2) * LANES
        near, far = (96, 32) if f % 2 == 0 else (32, 96)
        rolled = []
        for x in range(2):
            taps = jnp.where(low_half == (f % 2 == 0), band_ref[x, :, at : at + LANES], 0.0)
            skewed = pltpu.roll(taps, 0, 1, stride=1, stride_axis=0)
            for base in (near, far):
                rolled.append(pltpu.roll(skewed, shift + base, 1))
        real, real_far, imag, imag_far = rolled
        own = jnp.concatenate(
            [jnp.where(low_half, real, -imag_far), jnp.where(low_half, imag, real_far)], axis=0
        )
        halo = jnp.concatenate(
            [jnp.where(low_half, real_far, -imag), jnp.where(low_half, imag_far, real)], axis=0
        )
        halo = jnp.concatenate(
            [jnp.where(from_left, halo, 0.0), jnp.where(from_left, 0.0, halo)], axis=1
        )
        own = split(own)
        oh_ref[f], ol_ref[f] = own
        hh_ref[f], hl_ref[f] = split(halo)
        waves = [wave_ref[x, f] for x in range(2)]
        squares = jnp.sum(waves[0] * waves[0] + waves[1] * waves[1], axis=0, keepdims=True)
        energy_ref[f : f + 1, :] = squares[:, :LANES] + squares[:, LANES:]
        masked = jnp.concatenate([w * mask for w in waves], axis=0)
        pred_ref[f] = product(own, split(masked))


def finish_kernel(
    taper_ref, pred_ref, oh_ref, ol_ref, hh_ref, hl_ref, left_ref, right_ref, after_ref, before_ref, lends_ref,
    rends_ref, mult_ref, energy_ref, ends_ref,
):
    gap = jnp.zeros((BLOCK - HALO, pred_ref.shape[2]), F32)
    lane = iota((2 * BLOCK, LANES), 1)
    weights = [taper_ref[u] for u in range(2 * SHALF + 1)]
    row = iota((8, 3 * LANES), 0)
    ends_ref[...] = jnp.zeros_like(ends_ref)
    middle = jnp.zeros((LANES - 16, 3 * LANES), F32)
    for f in range(pred_ref.shape[0]):
        at = slice(f * LANES, (f + 1) * LANES)
        window = jnp.concatenate(
            [gap, left_ref[0, f], gap, left_ref[1, f], right_ref[0, f], gap, right_ref[1, f], gap], axis=0
        )
        halo = (hh_ref[f], hl_ref[f])
        pred = pred_ref[f] + product(halo, split(window))
        for part, (first, last) in enumerate(
            [
                (after_ref[:, at], before_ref[:, at]),
                (lends_ref[:SHALF, at], lends_ref[SHALF:, at]),
                (rends_ref[:SHALF, at], rends_ref[SHALF:, at]),
            ]
        ):
            ends_ref[f, :SHALF, part * LANES : (part + 1) * LANES] = first
            ends_ref[f, 8 - SHALF :, part * LANES : (part + 1) * LANES] = last
        ends = ends_ref[f]
        ends = jnp.concatenate(
            [jnp.where(row < SHALF, ends, 0.0), middle, jnp.where(row >= 8 - SHALF, ends, 0.0)], axis=0
        )
        band = tuple(
            jnp.concatenate([own_ref[f], halo_ref[f]], axis=1)
            for own_ref, halo_ref in ((oh_ref, hh_ref), (ol_ref, hl_ref))
        )
        edge = product(band, split(ends), transposed=True)
        head, tail = pred[:, :LANES], pred[:, LANES:]
        shots = pred.shape[1]
        total = weights[SHALF] * pred
        for u in range(1, SHALF + 1):
            earlier = jnp.concatenate([head, jnp.where(lane >= LANES - u, edge, tail)], axis=1)
            later = jnp.concatenate([jnp.where(lane < u, edge, head), tail], axis=1)
            total = total + weights[SHALF - u] * pltpu.roll(earlier, u, 1)
            total = total + weights[SHALF + u] * pltpu.roll(later, shots - u, 1)
        mult_ref[0, f] = total[:BLOCK]
        mult_ref[1, f] = total[BLOCK:]
        squares = jnp.sum(total * total, axis=0, keepdims=True)
        energy_ref[f : f + 1, :] = squares[:, :LANES] + squares[:, LANES:]


def subtract_kernel(total_ref, wave_ref, mult_ref, out_ref):
    slices = wave_ref.shape[1]
    sums = jnp.sum(total_ref[...], axis=0, keepdims=True)
    lane = iota((1, LANES), 1)
    first = pl.program_id(0) * slices
    count = pl.num_programs(0) * slices
    for f in range(slices):
        data = jnp.sum(jnp.where(lane == first + f, sums, 0.0), axis=1, keepdims=True)
        pred = jnp.sum(jnp.where(lane == first + f + count, sums, 0.0), axis=1, keepdims=True)
        gain = jnp.sqrt((data + 1e-06) / (pred + 1e-06))
        for x in range(2):
            out_ref[x, f] = wave_ref[x, f] - gain * mult_ref[x, f]


def cells(slices, rows, shots):
    return pl.BlockSpec((2, slices, rows, shots), lambda i: (0, i, 0, 0))


def stacked(slices, rows, columns):
    return pl.BlockSpec((slices, rows, columns), lambda i: (i, 0, 0))


def lanes(rows, slices):
    return pl.BlockSpec((rows, slices * LANES), lambda i: (0, i))


SMEM = pl.BlockSpec(memory_space=pltpu.SMEM)


def whole(shape):
    return pl.BlockSpec(shape, lambda i: (0,) * len(shape))


def call(kernel, steps, in_specs, outs, name, flops, scratch=()):
    return pl.pallas_call(
        kernel,
        grid=(steps,),
        in_specs=in_specs,
        out_specs=[spec for spec, _, _ in outs],
        out_shape=[jax.ShapeDtypeStruct(shape, dtype) for _, shape, dtype in outs],
        scratch_shapes=list(scratch),
        name=name,
        cost_estimate=pl.CostEstimate(flops=flops, transcendentals=0, bytes_accessed=1 << 20),
        compiler_params=pltpu.CompilerParams(dimension_semantics=("arbitrary",)),
    )


def neighbours(axis):
    count = lax.axis_size(axis)
    up = [(i, i + 1) for i in range(count - 1)]
    return up, [(j, i) for i, j in up]


def per_device(wavefield, surface_band, band_shift, trace_mask, shot_taper):
    _, slices, receivers, shots = wavefield.shape
    rcv_up, rcv_down = neighbours(RCV)
    src_up, src_down = neighbours(SRC)
    mask = trace_mask.reshape(1, receivers)

    step = 4
    steps = slices // step
    to_left, to_right, first, last = call(
        prepare_kernel,
        steps,
        [cells(step, receivers, shots), whole((1, receivers))],
        [
            (cells(step, HALO, shots), (2, slices, HALO, shots), F32),
            (cells(step, HALO, shots), (2, slices, HALO, shots), F32),
            (lanes(SHALF, step), (SHALF, slices * LANES), F32),
            (lanes(SHALF, step), (SHALF, slices * LANES), F32),
        ],
        "prepare",
        1 << 20,
    )(wavefield, mask)
    from_right = lax.ppermute(to_left, RCV, rcv_down)
    from_left = lax.ppermute(to_right, RCV, rcv_up)
    after = lax.ppermute(first, SRC, src_down)
    before = lax.ppermute(last, SRC, src_up)
    ends = jnp.concatenate([after, before], axis=0)
    right_ends = lax.ppermute(ends, RCV, rcv_down)
    left_ends = lax.ppermute(ends, RCV, rcv_up)

    matrix = 2 * receivers
    own_high, own_low, halo_high, halo_low, predicted, data_energy = call(
        own_kernel,
        2,
        [
            SMEM,
            cells(8, receivers, shots),
            whole((1, receivers)),
            pl.BlockSpec((2, receivers, 8 * APER), lambda i: (0, 0, i)),
        ],
        [
            (stacked(8, matrix, LANES), (slices, matrix, LANES), BF16),
            (stacked(8, matrix, LANES), (slices, matrix, LANES), BF16),
            (stacked(8, matrix, 2 * LANES), (slices, matrix, 2 * LANES), BF16),
            (stacked(8, matrix, 2 * LANES), (slices, matrix, 2 * LANES), BF16),
            (stacked(8, matrix, shots), (slices, matrix, shots), F32),
            (pl.BlockSpec((8, LANES), lambda i: (i, 0)), (slices, LANES), F32),
        ],
        "own",
        1 << 28,
    )(band_shift, wavefield, mask, surface_band)

    multiples, pred_energy = call(
        finish_kernel,
        2,
        [
            SMEM,
            stacked(8, matrix, shots),
            stacked(8, matrix, LANES),
            stacked(8, matrix, LANES),
            stacked(8, matrix, 2 * LANES),
            stacked(8, matrix, 2 * LANES),
            cells(8, HALO, shots),
            cells(8, HALO, shots),
            lanes(SHALF, 8),
            lanes(SHALF, 8),
            lanes(2 * SHALF, 8),
            lanes(2 * SHALF, 8),
        ],
        [
            (cells(8, receivers, shots), (2, slices, receivers, shots), F32),
            (pl.BlockSpec((8, LANES), lambda i: (i, 0)), (slices, LANES), F32),
        ],
        "finish",
        1 << 28,
        [pltpu.VMEM((8, 8, 3 * LANES), F32)],
    )(
        shot_taper, predicted, own_high, own_low, halo_high, halo_low, from_left, from_right, after, before,
        left_ends, right_ends,
    )

    partial = jnp.sum(jnp.concatenate([data_energy, pred_energy], axis=0), axis=1)[None, None]
    partial = jnp.pad(partial, ((0, 0), (0, 0), (0, LANES - partial.shape[2])))
    devices = lax.axis_size(SRC_RCV)
    spread = jnp.broadcast_to(partial, (devices, 1, LANES))
    energies = lax.all_to_all(spread, SRC_RCV, 0, 0, tiled=True).reshape(devices, LANES)

    (primaries,) = call(
        subtract_kernel,
        steps,
        [whole((devices, LANES)), cells(step, receivers, shots), cells(step, receivers, shots)],
        [(cells(step, receivers, shots), (2, slices, receivers, shots), F32)],
        "subtract",
        1 << 20,
    )(energies, wavefield, multiples)
    return (multiples, primaries)


def solution(mesh):
    split_mesh = Mesh(
        mesh.devices.reshape(4, 2, 2, 8, 2), ("src_0", "src_1", "rcv_0", "rcv_1", "rcv_2")
    )
    return jax.shard_map(
        per_device,
        mesh=split_mesh,
        in_specs=(P(None, None, RCV, SRC), P(None, RCV, None), P(RCV), P(RCV), P()),
        out_specs=(P(None, None, RCV, SRC), P(None, None, RCV, SRC)),
        check_vma=False,
    )
```

```python
import functools

import jax
import jax.numpy as jnp
from jax import lax
from jax.experimental import pallas as pl
from jax.experimental.pallas import tpu as pltpu
from jax.sharding import Mesh
from jax.sharding import PartitionSpec as P

APER = 64
SHIFT = 16
BLOCK = 64
SHALF = 2
HALO = APER // 2 + SHIFT
SPARE = BLOCK - HALO
LANES = 128
RCV = ("rcv_0", "rcv_1", "rcv_2")
SRC = ("src_0", "src_1")
SRC_RCV = ("src_0", "src_1", "rcv_0", "rcv_1", "rcv_2")
F32 = jnp.float32
BF16 = jnp.bfloat16
FIRST = 11
KEPT = 8


def iota(shape, dim):
    return lax.broadcasted_iota(jnp.int32, shape, dim)


def split(x):
    high = x.astype(BF16)
    return high, (x - high.astype(F32)).astype(BF16)


def product(a, b):
    dot = functools.partial(jnp.dot, preferred_element_type=F32)
    return dot(a[0], b[0]) + (dot(a[0], b[1]) + dot(a[1], b[0]))


def mask_column(mask_ref):
    row = jnp.broadcast_to(mask_ref[...].astype(F32), (BLOCK, BLOCK))
    diagonal = iota((BLOCK, BLOCK), 0) == iota((BLOCK, BLOCK), 1)
    return jnp.sum(jnp.where(diagonal, row, 0.0), axis=1, keepdims=True)


def is_odd():
    return lax.axis_index("rcv_2") == 1


def at_end(column, tail):
    return jnp.where(tail, column[SPARE:], column[:HALO])


def head_kernel(wave_ref, mask_ref, out_ref, held_ref, sems):
    tail = is_odd()
    start = pl.multiple_of(jnp.where(tail, SPARE, 0), 8)
    slices = wave_ref.shape[1]
    copies = []
    for i, (low, high) in enumerate([(0, FIRST), (FIRST, slices)]):
        part = pl.ds(low, high - low)
        copies.append(pltpu.make_async_copy(wave_ref.at[:, part], held_ref.at[:, part], sems.at[i]))
        copies[-1].start()
    mask = at_end(mask_column(mask_ref), tail)
    copies[0].wait()
    for x in range(2):
        for f in range(FIRST):
            out_ref[x, f] = held_ref[x, f, pl.ds(start, HALO)] * mask
    copies[1].wait()


def rest_kernel(wave_ref, mask_ref, link_ref, chip_ref, ends_ref):
    odd = is_odd()
    mask = mask_column(mask_ref)
    lane = iota((BLOCK, LANES), 1)
    slices = wave_ref.shape[1]
    ends = jnp.zeros((BLOCK, LANES), F32)
    for f in range(slices):
        for x in range(2):
            masked = wave_ref[x, f] * mask
            place = 4 * (x * slices + f)
            row = (2 * f + x) * HALO
            chip_ref[row : row + HALO] = at_end(masked, jnp.logical_not(odd))
            if f >= FIRST:
                row -= 2 * FIRST * HALO
                link_ref[row : row + HALO] = at_end(masked, odd)
            last = pltpu.roll(masked[:, -LANES:], (place + SHALF) % LANES, 1)
            first = pltpu.roll(masked[:, :LANES], place + SHALF, 1)
            ends = jnp.where(lane // 2 == place // 2, last, ends)
            ends = jnp.where(lane // 2 == place // 2 + 1, first, ends)
    ends_ref[...] = ends


def merged_ends(before_ref, after_ref):
    return jnp.where(iota((BLOCK, LANES), 1) % 4 < SHALF, before_ref[...], after_ref[...])


def pack_kernel(before_ref, after_ref, _link_in, _chip_in, link_ref, chip_ref):
    odd = is_odd()
    ends = merged_ends(before_ref, after_ref)
    for ref, tail in ((link_ref, odd), (chip_ref, jnp.logical_not(odd))):
        rows = at_end(ends, tail)
        ref[ref.shape[0] - HALO // 2 :] = jnp.concatenate([rows[: HALO // 2], rows[HALO // 2 :]], axis=1)


def band_kernel(shift_ref, wave_ref, band_ref, high_ref, low_ref, energy_ref):
    shift = shift_ref[0]
    odd = is_odd()
    low_half = iota((BLOCK, LANES), 1) < APER
    left = iota((2 * BLOCK, LANES), 0) % BLOCK + shift < APER // 2
    on_chip = left == odd
    for f in range(wave_ref.shape[1]):
        at = (f // 2) * LANES
        near, far = (96, 32) if f % 2 == 0 else (32, 96)
        rolled = []
        for x in range(2):
            taps = jnp.where(low_half == (f % 2 == 0), band_ref[x, :, at : at + LANES], 0.0)
            skewed = pltpu.roll(taps, 0, 1, stride=1, stride_axis=0)
            for base in (near, far):
                rolled.append(pltpu.roll(skewed, shift + base, 1))
        real, real_far, imag, imag_far = rolled
        own = jnp.concatenate(
            [jnp.where(low_half, real, -imag_far), jnp.where(low_half, imag, real_far)], axis=0
        )
        halo = jnp.concatenate(
            [jnp.where(low_half, real_far, -imag), jnp.where(low_half, imag_far, real)], axis=0
        )
        halo = jnp.where(left, pltpu.roll(halo, LANES - SPARE, 1), halo)
        parts = [own, jnp.where(on_chip, halo, 0.0), jnp.where(on_chip, 0.0, halo)]
        for part, value in enumerate(parts):
            high, low = split(value)
            high_ref[f, :, part * LANES : (part + 1) * LANES] = high
            low_ref[f, :, part * LANES : (part + 1) * LANES] = low
        squares = wave_ref[0, f] * wave_ref[0, f] + wave_ref[1, f] * wave_ref[1, f]
        squares = jnp.sum(squares, axis=0, keepdims=True)
        energy_ref[f : f + 1, :] = squares[:, :LANES] + squares[:, LANES:]


def finish_kernel(
    taper_ref, wave_ref, mask_ref, high_ref, low_ref, head_ref, link_ref, chip_ref, before_ref, after_ref, data_ref,
    mult_ref, spread_ref, kept_ref,
):
    slices = wave_ref.shape[1]
    shots = wave_ref.shape[3]
    mask = mask_column(mask_ref)
    lane = iota((2 * BLOCK, LANES), 1)
    weights = [taper_ref[u] for u in range(2 * SHALF + 1)]
    gap = jnp.zeros((SPARE, shots + LANES), F32)

    def unpacked(ref):
        rows = ref[ref.shape[0] - HALO // 2 :]
        return jnp.concatenate([rows[:, :LANES], rows[:, LANES:]], axis=0)

    ends = merged_ends(before_ref, after_ref)
    link_ends = unpacked(link_ref)
    chip_ends = unpacked(chip_ref)
    row = iota((1, LANES), 1)
    energies = jnp.zeros((1, LANES), F32)
    for f in range(slices):
        pieces = []
        for source in range(3):
            for x in range(2):
                place = LANES - (4 * (x * slices + f) + SHALF)
                at = (2 * f + x) * HALO
                if source == 0:
                    pieces.append(jnp.concatenate([wave_ref[x, f] * mask, pltpu.roll(ends, place, 1)], axis=1))
                    continue
                if source == 1:
                    main, edge = chip_ref[at : at + HALO], chip_ends
                elif f < FIRST:
                    main, edge = head_ref[x, f], link_ends
                else:
                    at -= 2 * FIRST * HALO
                    main, edge = link_ref[at : at + HALO], link_ends
                pieces.append(jnp.concatenate([main, pltpu.roll(edge, place, 1)], axis=1))
                pieces.append(gap)
        whole = product((high_ref[f], low_ref[f]), split(jnp.concatenate(pieces, axis=0)))
        pred, edge = whole[:, :shots], whole[:, shots:]
        head, tail = pred[:, :LANES], pred[:, LANES:]
        total = weights[SHALF] * pred
        for u in range(1, SHALF + 1):
            earlier = jnp.concatenate([head, jnp.where(lane >= LANES - u, edge, tail)], axis=1)
            later = jnp.concatenate([jnp.where(lane < u, edge, head), tail], axis=1)
            total = total + weights[SHALF - u] * pltpu.roll(earlier, u, 1)
            total = total + weights[SHALF + u] * pltpu.roll(later, shots - u, 1)
        mult_ref[0, f] = total[:BLOCK]
        mult_ref[1, f] = total[BLOCK:]
        squares = jnp.sum(total * total, axis=0, keepdims=True)
        pred_energy = jnp.sum(squares[:, :LANES] + squares[:, LANES:], axis=1, keepdims=True)
        data_energy = jnp.sum(data_ref[f : f + 1, :], axis=1, keepdims=True)
        energies = jnp.where(row == f, data_energy, energies)
        energies = jnp.where(row == slices + f, pred_energy, energies)
    spread_ref[...] = jnp.broadcast_to(energies, spread_ref.shape)
    kept_ref[...] = wave_ref[:, :KEPT]


def subtract_kernel(total_ref, kept_ref, wave_ref, mult_ref, out_ref, held_ref, in_sems, out_sems):
    slices = wave_ref.shape[1]
    reads = {}
    for f in range(KEPT, slices):
        reads[f] = pltpu.make_async_copy(wave_ref.at[:, f], held_ref.at[:, f], in_sems.at[f])
        reads[f].start()
    sums = jnp.sum(total_ref[...], axis=0, keepdims=True)
    row = iota((1, LANES), 1)
    writes = []
    for f in range(slices):
        data = jnp.sum(jnp.where(row == f, sums, 0.0), axis=1, keepdims=True)
        pred = jnp.sum(jnp.where(row == slices + f, sums, 0.0), axis=1, keepdims=True)
        gain = jnp.sqrt((data + 1e-06) / (pred + 1e-06))
        if f in reads:
            reads[f].wait()
        source_ref = held_ref if f in reads else kept_ref
        for x in range(2):
            held_ref[x, f] = source_ref[x, f] - gain * mult_ref[x, f]
        writes.append(pltpu.make_async_copy(held_ref.at[:, f], out_ref.at[:, f], out_sems.at[f]))
        writes[-1].start()
    for copy in writes:
        copy.wait()


VMEM = pl.BlockSpec(memory_space=pltpu.VMEM)
SMEM = pl.BlockSpec(memory_space=pltpu.SMEM)
HBM = pl.BlockSpec(memory_space=pltpu.HBM)
ANY = pl.BlockSpec(memory_space=pl.ANY)


def on_chip(*arrays):
    return [pltpu.with_memory_space_constraint(a, pltpu.VMEM) for a in arrays]


def call(kernel, in_specs, out_shapes, flops, out_specs=None, scratch=(), aliases=None):
    return pl.pallas_call(
        kernel,
        in_specs=in_specs,
        out_specs=out_specs or [VMEM] * len(out_shapes),
        out_shape=out_shapes,
        scratch_shapes=list(scratch),
        input_output_aliases=aliases or {},
        cost_estimate=pl.CostEstimate(flops=flops, transcendentals=0, bytes_accessed=1 << 20),
        compiler_params=pltpu.CompilerParams(vmem_limit_bytes=24 << 20),
    )


def neighbours(axis):
    count = lax.axis_size(axis)
    up = [(i, i + 1) for i in range(count - 1)]
    return up, [(j, i) for i, j in up]


def swaps(axis, first):
    count = lax.axis_size(axis)
    pairs = [(i, i + 1) for i in range(first, count - 1, 2)]
    return pairs + [(j, i) for i, j in pairs]


def per_device(wavefield, surface_band, band_shift, trace_mask, shot_taper):
    _, slices, receivers, shots = wavefield.shape
    src_up, src_down = neighbours(SRC)
    mask = trace_mask.reshape(1, receivers)
    devices = lax.axis_size(SRC_RCV)
    in_hbm = pltpu.with_memory_space_constraint(wavefield, pltpu.HBM)

    head, wave = call(
        head_kernel,
        [HBM, VMEM],
        [
            pltpu.VMEM((2, FIRST, HALO, shots), F32),
            pltpu.VMEM((2, slices, receivers, shots), F32),
        ],
        1 << 20,
        scratch=[pltpu.SemaphoreType.DMA((2,))],
    )(in_hbm, mask)
    head = lax.ppermute(head, RCV, swaps(RCV, 1))

    wave, band = on_chip(wave, surface_band)
    link, chip, ends = call(
        rest_kernel,
        [VMEM, VMEM],
        [
            pltpu.VMEM((2 * (slices - FIRST) * HALO + HALO // 2, shots), F32),
            pltpu.VMEM((2 * slices * HALO + HALO // 2, shots), F32),
            pltpu.VMEM((BLOCK, LANES), F32),
        ],
        1 << 20,
    )(wave, mask)
    after = lax.ppermute(ends, SRC, src_down)
    before = lax.ppermute(ends, SRC, src_up)

    rows = 2 * receivers
    high, low, data_energy = call(
        band_kernel,
        [SMEM, VMEM, VMEM],
        [
            pltpu.VMEM((slices, rows, 3 * LANES), BF16),
            pltpu.VMEM((slices, rows, 3 * LANES), BF16),
            pltpu.VMEM((slices, LANES), F32),
        ],
        1 << 28,
    )(band_shift, wave, band)

    before, after, link, chip = on_chip(before, after, link, chip)
    link, chip = call(
        pack_kernel,
        [VMEM, VMEM, ANY, ANY],
        [pltpu.VMEM(link.shape, F32), pltpu.VMEM(chip.shape, F32)],
        1 << 16,
        aliases={2: 0, 3: 1},
    )(before, after, link, chip)
    link = lax.ppermute(link, RCV, swaps(RCV, 1))
    chip = lax.ppermute(chip, RCV, swaps(RCV, 0))

    multiples, spread, kept = call(
        finish_kernel,
        [SMEM] + [VMEM] * 10,
        [
            pltpu.VMEM((2, slices, receivers, shots), F32),
            pltpu.VMEM((devices, LANES), F32),
            pltpu.VMEM((2, KEPT, receivers, shots), F32),
        ],
        1 << 28,
    )(shot_taper, wave, mask, *on_chip(high, low, head, link, chip), before, after, *on_chip(data_energy))

    energies = lax.all_to_all(spread[:, None], SRC_RCV, 0, 0, tiled=True).reshape(devices, LANES)

    (primaries,) = call(
        subtract_kernel,
        [VMEM, VMEM, HBM, VMEM],
        [jax.ShapeDtypeStruct((2, slices, receivers, shots), F32)],
        1 << 20,
        out_specs=[HBM],
        scratch=[pltpu.VMEM((2, slices, receivers, shots), F32)] + [pltpu.SemaphoreType.DMA((slices,))] * 2,
    )(*on_chip(energies, kept), in_hbm, *on_chip(multiples))
    return (multiples, primaries)


def solution(mesh):
    split_mesh = Mesh(
        mesh.devices.reshape(4, 2, 2, 8, 2), ("src_0", "src_1", "rcv_0", "rcv_1", "rcv_2")
    )
    return jax.shard_map(
        per_device,
        mesh=split_mesh,
        in_specs=(P(None, None, RCV, SRC), P(None, RCV, None), P(RCV), P(RCV), P()),
        out_specs=(P(None, None, RCV, SRC), P(None, None, RCV, SRC)),
        check_vma=False,
    )
```

```python
import functools

import jax
import jax.numpy as jnp
from jax import lax
from jax.experimental import pallas as pl
from jax.experimental.pallas import tpu as pltpu
from jax.sharding import Mesh
from jax.sharding import PartitionSpec as P

APER = 64
SHIFT = 16
BLOCK = 64
SHALF = 2
HALO = APER // 2 + SHIFT
SPARE = BLOCK - HALO
LANES = 128
RCV = ("rcv_0", "rcv_1", "rcv_2")
SRC = ("src_0", "src_1")
SRC_RCV = ("src_0", "src_1", "rcv_0", "rcv_1", "rcv_2")
F32 = jnp.float32
BF16 = jnp.bfloat16
FIRST = 14
KEPT = 8


def iota(shape, dim):
    return lax.broadcasted_iota(jnp.int32, shape, dim)


def split(x):
    high = x.astype(BF16)
    return high, (x - high.astype(F32)).astype(BF16)


def product(a, b):
    dot = functools.partial(jnp.dot, preferred_element_type=F32)
    return dot(a[0], b[0]) + (dot(a[0], b[1]) + dot(a[1], b[0]))


def mask_column(mask_ref):
    row = jnp.broadcast_to(mask_ref[...].astype(F32), (BLOCK, BLOCK))
    diagonal = iota((BLOCK, BLOCK), 0) == iota((BLOCK, BLOCK), 1)
    return jnp.sum(jnp.where(diagonal, row, 0.0), axis=1, keepdims=True)


def is_odd():
    return lax.axis_index("rcv_2") == 1


def at_end(column, tail):
    return jnp.where(tail, column[SPARE:], column[:HALO])


def head_kernel(wave_ref, mask_ref, out_ref, held_ref, live_ref, sems):
    tail = is_odd()
    start = pl.multiple_of(jnp.where(tail, SPARE, 0), 8)
    slices = wave_ref.shape[1]
    copies = [pltpu.make_async_copy(mask_ref, live_ref, sems.at[2])]
    for i, (low, high) in enumerate([(0, FIRST), (FIRST, slices)]):
        part = pl.ds(low, high - low)
        copies.append(pltpu.make_async_copy(wave_ref.at[:, part], held_ref.at[:, part], sems.at[i]))
    for copy in copies:
        copy.start()
    copies[0].wait()
    mask = at_end(mask_column(live_ref), tail)
    copies[1].wait()
    for x in range(2):
        for f in range(FIRST):
            out_ref[x, f] = held_ref[x, f, pl.ds(start, HALO)] * mask
    copies[2].wait()


def rest_kernel(wave_ref, mask_ref, link_ref, chip_ref, ends_ref):
    odd = is_odd()
    mask = mask_column(mask_ref)
    lane = iota((BLOCK, LANES), 1)
    slices = wave_ref.shape[1]
    ends = jnp.zeros((BLOCK, LANES), F32)
    for f in range(slices):
        for x in range(2):
            masked = wave_ref[x, f] * mask
            place = 4 * (x * slices + f)
            row = (2 * f + x) * HALO
            chip_ref[row : row + HALO] = at_end(masked, jnp.logical_not(odd))
            if f >= FIRST:
                row -= 2 * FIRST * HALO
                link_ref[row : row + HALO] = at_end(masked, odd)
            last = pltpu.roll(masked[:, -LANES:], (place + SHALF) % LANES, 1)
            first = pltpu.roll(masked[:, :LANES], place + SHALF, 1)
            ends = jnp.where(lane // 2 == place // 2, last, ends)
            ends = jnp.where(lane // 2 == place // 2 + 1, first, ends)
    ends_ref[...] = ends


def merged_ends(before_ref, after_ref):
    return jnp.where(iota((BLOCK, LANES), 1) % 4 < SHALF, before_ref[...], after_ref[...])


def pack_kernel(before_ref, after_ref, _link_in, _chip_in, link_ref, chip_ref):
    odd = is_odd()
    ends = merged_ends(before_ref, after_ref)
    for ref, tail in ((link_ref, odd), (chip_ref, jnp.logical_not(odd))):
        rows = at_end(ends, tail)
        ref[ref.shape[0] - HALO // 2 :] = jnp.concatenate([rows[: HALO // 2], rows[HALO // 2 :]], axis=1)


def band_kernel(wave_ref, band_ref, high_ref, low_ref, energy_ref):
    low_half = iota((BLOCK, LANES), 1) < APER
    for f in range(wave_ref.shape[1]):
        at = (f // 2) * LANES
        skewed = []
        for x in range(2):
            taps = jnp.where(low_half == (f % 2 == 0), band_ref[x, :, at : at + LANES], 0.0)
            skewed.append(pltpu.roll(taps, APER * (f % 2), 1, stride=1, stride_axis=0))
        real, imag = skewed
        for row, parts in enumerate([(real, -imag), (imag, real)]):
            for column, part in enumerate(parts):
                place = (f, slice(row * BLOCK, (row + 1) * BLOCK), slice(column * LANES, (column + 1) * LANES))
                high_ref[place], low_ref[place] = split(part)
        squares = wave_ref[0, f] * wave_ref[0, f] + wave_ref[1, f] * wave_ref[1, f]
        squares = jnp.sum(squares, axis=0, keepdims=True)
        energy_ref[f : f + 1, :] = squares[:, :LANES] + squares[:, LANES:]


def framed(frame_ref, own, chip, link, start):
    odd = is_odd()
    left, right = 0, HALO + BLOCK
    frame_ref[HALO : HALO + BLOCK] = own
    frame_ref[pl.ds(pl.multiple_of(jnp.where(odd, left, right), 8), HALO)] = chip
    frame_ref[pl.ds(pl.multiple_of(jnp.where(odd, right, left), 8), HALO)] = link
    return frame_ref[pl.ds(start, LANES)]


def window(frames_ref, wave_ref, mask, chip_ref, link, f, start):
    rows = []
    for x in range(2):
        own = wave_ref[x, f] * mask
        at = (2 * f + x) * HALO
        chip = chip_ref[at : at + HALO]
        other = link(x)
        columns = []
        for tile in range(own.shape[1] // LANES):
            part = slice(tile * LANES, (tile + 1) * LANES)
            columns.append(framed(frames_ref.at[x, tile], own[:, part], chip[:, part], other[:, part], start))
        rows.append(jnp.concatenate(columns, axis=1))
    return jnp.concatenate(rows, axis=0)


def gather_kernel(shift_ref, wave_ref, mask_ref, high_ref, low_ref, head_ref, chip_ref, pred_ref, frames_ref):
    start = SPARE + shift_ref[0]
    mask = mask_column(mask_ref)
    for f in range(FIRST):
        data = window(frames_ref.at[f], wave_ref, mask, chip_ref, lambda x, f=f: head_ref[x, f], f, start)
        pred_ref[f] = product((high_ref[f], low_ref[f]), split(data))


def finish_kernel(
    shift_ref, taper_ref, wave_ref, mask_ref, high_ref, low_ref, pred_ref, link_ref, chip_ref, before_ref, after_ref,
    data_ref, mult_ref, spread_ref, kept_ref, frames_ref, edges_ref,
):
    start = SPARE + shift_ref[0]
    slices = wave_ref.shape[1]
    shots = wave_ref.shape[3]
    mask = mask_column(mask_ref)
    lane = iota((2 * BLOCK, LANES), 1)
    weights = [taper_ref[u] for u in range(2 * SHALF + 1)]

    def unpacked(ref):
        rows = ref[ref.shape[0] - HALO // 2 :]
        return jnp.concatenate([rows[:, :LANES], rows[:, LANES:]], axis=0)

    ends = framed(
        frames_ref.at[slices - FIRST, 0, 0], merged_ends(before_ref, after_ref), unpacked(chip_ref), unpacked(link_ref),
        start,
    )
    ends = split(ends)
    rows = 2 * BLOCK * slices
    for x in range(2):
        part = slice(x * LANES, (x + 1) * LANES)
        matrices = tuple(ref[:, :, part].reshape(rows, LANES) for ref in (high_ref, low_ref))
        edges_ref[x] = product(matrices, ends).reshape(slices, 2 * BLOCK, LANES)

    def linked(x, f):
        at = (2 * (f - FIRST) + x) * HALO
        return link_ref[at : at + HALO]

    row = iota((1, LANES), 1)
    energies = jnp.zeros((1, LANES), F32)
    for f in range(slices):
        if f < FIRST:
            pred = pred_ref[f]
        else:
            frames = frames_ref.at[f - FIRST]
            data = window(frames, wave_ref, mask, chip_ref, lambda x, f=f: linked(x, f), f, start)
            pred = product((high_ref[f], low_ref[f]), split(data))
        edge = sum(
            pltpu.roll(edges_ref[x, f], LANES - (4 * (x * slices + f) + SHALF), 1) for x in range(2)
        )
        head, tail = pred[:, :LANES], pred[:, LANES:]
        total = weights[SHALF] * pred
        for u in range(1, SHALF + 1):
            earlier = jnp.concatenate([head, jnp.where(lane >= LANES - u, edge, tail)], axis=1)
            later = jnp.concatenate([jnp.where(lane < u, edge, head), tail], axis=1)
            total = total + weights[SHALF - u] * pltpu.roll(earlier, u, 1)
            total = total + weights[SHALF + u] * pltpu.roll(later, shots - u, 1)
        mult_ref[0, f] = total[:BLOCK]
        mult_ref[1, f] = total[BLOCK:]
        squares = jnp.sum(total * total, axis=0, keepdims=True)
        pred_energy = jnp.sum(squares[:, :LANES] + squares[:, LANES:], axis=1, keepdims=True)
        data_energy = jnp.sum(data_ref[f : f + 1, :], axis=1, keepdims=True)
        energies = jnp.where(row == f, data_energy, energies)
        energies = jnp.where(row == slices + f, pred_energy, energies)
    spread_ref[...] = jnp.broadcast_to(energies, spread_ref.shape)
    kept_ref[...] = wave_ref[:, :KEPT]


def subtract_kernel(total_ref, kept_ref, wave_ref, mult_ref, out_ref, held_ref, in_sems, out_sems):
    slices = wave_ref.shape[1]
    reads = {}
    for f in range(KEPT, slices):
        reads[f] = pltpu.make_async_copy(wave_ref.at[:, f], held_ref.at[:, f], in_sems.at[f])
        reads[f].start()
    sums = jnp.sum(total_ref[...], axis=0, keepdims=True)
    row = iota((1, LANES), 1)
    writes = []
    for f in range(slices):
        data = jnp.sum(jnp.where(row == f, sums, 0.0), axis=1, keepdims=True)
        pred = jnp.sum(jnp.where(row == slices + f, sums, 0.0), axis=1, keepdims=True)
        gain = jnp.sqrt((data + 1e-06) / (pred + 1e-06))
        if f in reads:
            reads[f].wait()
        source_ref = held_ref if f in reads else kept_ref
        for x in range(2):
            held_ref[x, f] = source_ref[x, f] - gain * mult_ref[x, f]
        writes.append(pltpu.make_async_copy(held_ref.at[:, f], out_ref.at[:, f], out_sems.at[f]))
        writes[-1].start()
    for copy in writes:
        copy.wait()


VMEM = pl.BlockSpec(memory_space=pltpu.VMEM)
SMEM = pl.BlockSpec(memory_space=pltpu.SMEM)
HBM = pl.BlockSpec(memory_space=pltpu.HBM)
ANY = pl.BlockSpec(memory_space=pl.ANY)


def on_chip(*arrays):
    return [pltpu.with_memory_space_constraint(a, pltpu.VMEM) for a in arrays]


def call(kernel, in_specs, out_shapes, flops, out_specs=None, scratch=(), aliases=None):
    return pl.pallas_call(
        kernel,
        in_specs=in_specs,
        out_specs=out_specs or [VMEM] * len(out_shapes),
        out_shape=out_shapes,
        scratch_shapes=list(scratch),
        input_output_aliases=aliases or {},
        cost_estimate=pl.CostEstimate(flops=flops, transcendentals=0, bytes_accessed=1 << 20),
        compiler_params=pltpu.CompilerParams(vmem_limit_bytes=24 << 20),
    )


def neighbours(axis):
    count = lax.axis_size(axis)
    up = [(i, i + 1) for i in range(count - 1)]
    return up, [(j, i) for i, j in up]


def swaps(axis, first):
    count = lax.axis_size(axis)
    pairs = [(i, i + 1) for i in range(first, count - 1, 2)]
    return pairs + [(j, i) for i, j in pairs]


def per_device(wavefield, surface_band, band_shift, trace_mask, shot_taper):
    _, slices, receivers, shots = wavefield.shape
    src_up, src_down = neighbours(SRC)
    mask = trace_mask.reshape(1, receivers)
    devices = lax.axis_size(SRC_RCV)
    in_hbm = pltpu.with_memory_space_constraint(wavefield, pltpu.HBM)

    head, wave = call(
        head_kernel,
        [HBM, HBM],
        [
            pltpu.VMEM((2, FIRST, HALO, shots), F32),
            pltpu.VMEM((2, slices, receivers, shots), F32),
        ],
        1 << 20,
        scratch=[pltpu.VMEM((1, receivers), jnp.int32), pltpu.SemaphoreType.DMA((3,))],
    )(in_hbm, pltpu.with_memory_space_constraint(mask, pltpu.HBM))
    head = lax.ppermute(head, RCV, swaps(RCV, 1))

    wave, band = on_chip(wave, surface_band)
    link, chip, ends = call(
        rest_kernel,
        [VMEM, VMEM],
        [
            pltpu.VMEM((2 * (slices - FIRST) * HALO + HALO // 2, shots), F32),
            pltpu.VMEM((2 * slices * HALO + HALO // 2, shots), F32),
            pltpu.VMEM((BLOCK, LANES), F32),
        ],
        1 << 20,
    )(wave, mask)
    after = lax.ppermute(ends, SRC, src_down)
    before = lax.ppermute(ends, SRC, src_up)

    before, after, link, chip = on_chip(before, after, link, chip)
    link, chip = call(
        pack_kernel,
        [VMEM, VMEM, ANY, ANY],
        [pltpu.VMEM(link.shape, F32), pltpu.VMEM(chip.shape, F32)],
        1 << 16,
        aliases={2: 0, 3: 1},
    )(before, after, link, chip)
    link = lax.ppermute(link, RCV, swaps(RCV, 1))
    chip = lax.ppermute(chip, RCV, swaps(RCV, 0))

    rows = 2 * receivers
    high, low, data_energy = call(
        band_kernel,
        [VMEM, VMEM],
        [
            pltpu.VMEM((slices, rows, 2 * LANES), BF16),
            pltpu.VMEM((slices, rows, 2 * LANES), BF16),
            pltpu.VMEM((slices, LANES), F32),
        ],
        1 << 28,
    )(wave, band)
    high, low, head, chip = on_chip(high, low, head, chip)
    frame = (2, shots // LANES, 2 * HALO + BLOCK, LANES)
    (predicted,) = call(
        gather_kernel,
        [SMEM] + [VMEM] * 6,
        [pltpu.VMEM((FIRST, rows, shots), F32)],
        1 << 28,
        scratch=[pltpu.VMEM((FIRST,) + frame, F32)],
    )(band_shift, wave, mask, high, low, head, chip)
    multiples, spread, kept = call(
        finish_kernel,
        [SMEM, SMEM] + [VMEM] * 10,
        [
            pltpu.VMEM((2, slices, receivers, shots), F32),
            pltpu.VMEM((devices, LANES), F32),
            pltpu.VMEM((2, KEPT, receivers, shots), F32),
        ],
        1 << 28,
        scratch=[
            pltpu.VMEM((slices - FIRST + 1,) + frame, F32),
            pltpu.VMEM((2, slices, rows, LANES), F32),
        ],
    )(
        band_shift, shot_taper, wave, mask, high, low, *on_chip(predicted, link), chip, before, after,
        *on_chip(data_energy),
    )

    energies = lax.all_to_all(spread[:, None], SRC_RCV, 0, 0, tiled=True).reshape(devices, LANES)

    (primaries,) = call(
        subtract_kernel,
        [VMEM, VMEM, HBM, VMEM],
        [jax.ShapeDtypeStruct((2, slices, receivers, shots), F32)],
        1 << 20,
        out_specs=[HBM],
        scratch=[pltpu.VMEM((2, slices, receivers, shots), F32)] + [pltpu.SemaphoreType.DMA((slices,))] * 2,
    )(*on_chip(energies, kept), in_hbm, *on_chip(multiples))
    return (multiples, primaries)


def solution(mesh):
    split_mesh = Mesh(
        mesh.devices.reshape(4, 2, 2, 8, 2), ("src_0", "src_1", "rcv_0", "rcv_1", "rcv_2")
    )
    return jax.shard_map(
        per_device,
        mesh=split_mesh,
        in_specs=(P(None, None, RCV, SRC), P(None, RCV, None), P(RCV), P(RCV), P()),
        out_specs=(P(None, None, RCV, SRC), P(None, None, RCV, SRC)),
        check_vma=False,
    )
```

```python
import functools

import jax
import jax.numpy as jnp
from jax import lax
from jax.experimental import pallas as pl
from jax.experimental.pallas import tpu as pltpu
from jax.sharding import Mesh
from jax.sharding import PartitionSpec as P

APER = 64
SHIFT = 16
BLOCK = 64
SHALF = 2
HALO = APER // 2 + SHIFT
SPARE = BLOCK - HALO
LANES = 128
RCV = ("rcv_0", "rcv_1", "rcv_2")
SRC = ("src_0", "src_1")
SRC_RCV = ("src_0", "src_1", "rcv_0", "rcv_1", "rcv_2")
F32 = jnp.float32
BF16 = jnp.bfloat16
FIRST = 14
KEPT = 8


def iota(shape, dim):
    return lax.broadcasted_iota(jnp.int32, shape, dim)


def split(x):
    high = x.astype(BF16)
    return high, (x - high.astype(F32)).astype(BF16)


def product(a, b):
    dot = functools.partial(jnp.dot, preferred_element_type=F32)
    return dot(a[0], b[0]) + (dot(a[0], b[1]) + dot(a[1], b[0]))


def mask_column(mask_ref):
    row = jnp.broadcast_to(mask_ref[...].astype(F32), (BLOCK, BLOCK))
    diagonal = iota((BLOCK, BLOCK), 0) == iota((BLOCK, BLOCK), 1)
    return jnp.sum(jnp.where(diagonal, row, 0.0), axis=1, keepdims=True)


def is_odd():
    return lax.axis_index("rcv_2") == 1


def at_end(column, tail):
    return jnp.where(tail, column[SPARE:], column[:HALO])


def head_kernel(wave_ref, mask_ref, held_ref, ends_ref, live_ref, sems):
    slices = wave_ref.shape[1]
    group = slices // 2
    copies = [pltpu.make_async_copy(mask_ref, live_ref, sems.at[2])]
    for i in range(2):
        part = pl.ds(i * group, group)
        copies.append(pltpu.make_async_copy(wave_ref.at[:, part], held_ref.at[:, part], sems.at[i]))
    for copy in copies:
        copy.start()
    copies[0].wait()
    mask = mask_column(live_ref)
    lane = iota((BLOCK, LANES), 1)
    ends = jnp.zeros((BLOCK, LANES), F32)
    for f in range(slices):
        if f % group == 0:
            copies[1 + f // group].wait()
        for x in range(2):
            place = 4 * (x * slices + f)
            last = pltpu.roll(held_ref[x, f, :, -LANES:], (place + SHALF) % LANES, 1)
            first = pltpu.roll(held_ref[x, f, :, :LANES], place + SHALF, 1)
            ends = jnp.where(lane // 2 == place // 2, last, ends)
            ends = jnp.where(lane // 2 == place // 2 + 1, first, ends)
    ends_ref[...] = ends * mask


def rest_kernel(wave_ref, mask_ref, head_ref, link_ref, chip_ref):
    odd = is_odd()
    mask = mask_column(mask_ref)
    slices = wave_ref.shape[1]
    for f in range(slices):
        for x in range(2):
            masked = wave_ref[x, f] * mask
            row = (2 * f + x) * HALO
            chip_ref[row : row + HALO] = at_end(masked, jnp.logical_not(odd))
            if f < FIRST:
                head_ref[row : row + HALO] = at_end(masked, odd)
            else:
                row -= 2 * FIRST * HALO
                link_ref[row : row + HALO] = at_end(masked, odd)


def merged_ends(before_ref, after_ref):
    return jnp.where(iota((BLOCK, LANES), 1) % 4 < SHALF, before_ref[...], after_ref[...])


def pack_kernel(before_ref, after_ref, _link_in, _chip_in, link_ref, chip_ref):
    odd = is_odd()
    ends = merged_ends(before_ref, after_ref)
    for ref, tail in ((link_ref, odd), (chip_ref, jnp.logical_not(odd))):
        rows = at_end(ends, tail)
        ref[ref.shape[0] - HALO // 2 :] = jnp.concatenate([rows[: HALO // 2], rows[HALO // 2 :]], axis=1)


def band_kernel(wave_ref, band_ref, high_ref, low_ref, energy_ref):
    low_half = iota((BLOCK, LANES), 1) < APER
    for f in range(wave_ref.shape[1]):
        at = (f // 2) * LANES
        skewed = []
        for x in range(2):
            taps = jnp.where(low_half == (f % 2 == 0), band_ref[x, :, at : at + LANES], 0.0)
            skewed.append(pltpu.roll(taps, APER * (f % 2), 1, stride=1, stride_axis=0))
        real, imag = skewed
        for row, parts in enumerate([(real, -imag), (imag, real)]):
            for column, part in enumerate(parts):
                place = (f, slice(row * BLOCK, (row + 1) * BLOCK), slice(column * LANES, (column + 1) * LANES))
                high_ref[place], low_ref[place] = split(part)
        squares = wave_ref[0, f] * wave_ref[0, f] + wave_ref[1, f] * wave_ref[1, f]
        squares = jnp.sum(squares, axis=0, keepdims=True)
        energy_ref[f : f + 1, :] = squares[:, :LANES] + squares[:, LANES:]


def framed(frame_ref, own, chip, link, start):
    odd = is_odd()
    left, right = 0, HALO + BLOCK
    frame_ref[HALO : HALO + BLOCK] = own
    frame_ref[pl.ds(pl.multiple_of(jnp.where(odd, left, right), 8), HALO)] = chip
    frame_ref[pl.ds(pl.multiple_of(jnp.where(odd, right, left), 8), HALO)] = link
    return frame_ref[pl.ds(start, LANES)]


def window(frames_ref, wave_ref, mask, chip_ref, link, f, start):
    rows = []
    for x in range(2):
        own = wave_ref[x, f] * mask
        at = (2 * f + x) * HALO
        chip = chip_ref[at : at + HALO]
        other = link(x)
        columns = []
        for tile in range(own.shape[1] // LANES):
            part = slice(tile * LANES, (tile + 1) * LANES)
            columns.append(framed(frames_ref.at[x, tile], own[:, part], chip[:, part], other[:, part], start))
        rows.append(jnp.concatenate(columns, axis=1))
    return jnp.concatenate(rows, axis=0)


def gather_kernel(
    shift_ref, taper_ref, wave_ref, mask_ref, high_ref, low_ref, head_ref, chip_ref, mult_ref, th_ref, tl_ref, frames_ref,
    ph_ref, pl_ref,
):
    start = SPARE + shift_ref[0]
    mask = mask_column(mask_ref)
    shots = wave_ref.shape[3]
    taper = split(weights_at(taper_ref, iota((shots, shots), 0) - iota((shots, shots), 1)))
    th_ref[...], tl_ref[...] = taper
    rows = 2 * BLOCK
    for f in range(FIRST):
        at = 2 * f * HALO
        data = window(
            frames_ref.at[f], wave_ref, mask, chip_ref, lambda x, at=at: head_ref[at + x * HALO : at + (x + 1) * HALO], f, start
        )
        part = slice(f * rows, (f + 1) * rows)
        ph_ref[part], pl_ref[part] = split(product((high_ref[f], low_ref[f]), split(data)))
    group = FIRST // 2
    for i in range(2):
        part = slice(i * group * rows, (i + 1) * group * rows)
        whole = product((ph_ref[part], pl_ref[part]), taper)
        mult_ref[i * group : (i + 1) * group] = whole.reshape(group, rows, shots)


def weights_at(taper_ref, ahead):
    weights = jnp.zeros(ahead.shape, F32)
    for u in range(2 * SHALF + 1):
        weights = jnp.where(ahead == u - SHALF, taper_ref[u], weights)
    return weights


def finish_kernel(
    shift_ref, taper_ref, wave_ref, mask_ref, high_ref, low_ref, part_ref, th_ref, tl_ref, link_ref, chip_ref, before_ref,
    after_ref, data_ref, out_ref, mult_ref, spread_ref, kept_ref, frames_ref, pred_ref, sems,
):
    start = SPARE + shift_ref[0]
    slices = wave_ref.shape[1]
    shots = wave_ref.shape[3]
    rows = 2 * BLOCK
    mask = mask_column(mask_ref)

    def linked(x, f):
        at = (2 * (f - FIRST) + x) * HALO
        return link_ref[at : at + HALO]

    def unpacked(ref):
        cells = ref[ref.shape[0] - HALO // 2 :]
        return jnp.concatenate([cells[:, :LANES], cells[:, LANES:]], axis=0)

    ends = framed(
        frames_ref.at[slices - FIRST, 0, 0], merged_ends(before_ref, after_ref), unpacked(chip_ref), unpacked(link_ref),
        start,
    )
    ends = split(ends)
    kind = iota((LANES, LANES), 0) % 4
    source = jnp.where(kind < SHALF, kind - SHALF, kind - SHALF + shots)
    target = iota((LANES, LANES), 1)
    target = jnp.where(target < LANES // 2, target, target + shots - LANES)
    reach = split(weights_at(taper_ref, source - target))
    for f in range(FIRST, slices):
        data = window(frames_ref.at[f - FIRST], wave_ref, mask, chip_ref, lambda x, f=f: linked(x, f), f, start)
        pred = split(product((high_ref[f], low_ref[f]), split(data)))
        pred_ref[f - FIRST] = product(pred, (th_ref[...], tl_ref[...]))
    near = iota((rows, LANES), 1) < LANES // 2
    squares = []
    writes = []
    group = 4
    for first in range(0, slices, group):
        shape = (group, rows, LANES)
        owner = iota(shape, 2) // 4 - iota(shape, 0) - first
        edge = jnp.zeros(shape, F32)
        for x in range(2):
            part = slice(x * LANES, (x + 1) * LANES)
            matrices = tuple(ref[first : first + group, :, part].reshape(group * rows, LANES) for ref in (high_ref, low_ref))
            edge = jnp.where(owner == x * slices, product(matrices, ends).reshape(shape), edge)
        edge = product(split(edge.reshape(group * rows, LANES)), reach)
        for f in range(first, first + group):
            own = part_ref[f] if f < FIRST else pred_ref[f - FIRST]
            extra = edge[(f - first) * rows : (f - first + 1) * rows]
            total = jnp.concatenate(
                [own[:, :LANES] + jnp.where(near, extra, 0.0), own[:, LANES:] + jnp.where(near, 0.0, extra)], axis=1
            )
            mult_ref[0, f] = total[:BLOCK]
            mult_ref[1, f] = total[BLOCK:]
            total = jnp.sum(total * total, axis=0, keepdims=True)
            squares.append(total[:, :LANES] + total[:, LANES:])
        part = pl.ds(first, group)
        writes.append(pltpu.make_async_copy(mult_ref.at[:, part], out_ref.at[:, part], sems.at[first // group]))
        writes[-1].start()
    lane = iota((slices, LANES), 1) - iota((slices, LANES), 0)
    row = iota((slices, LANES), 0)
    pred_rows = jnp.zeros((slices, LANES), F32)
    for f in range(slices):
        pred_rows = jnp.where(row == f, squares[f], pred_rows)
    pred_energy = jnp.sum(pred_rows, axis=1, keepdims=True)
    data_energy = jnp.sum(data_ref[...], axis=1, keepdims=True)
    energies = jnp.where(lane == 0, data_energy, jnp.where(lane == slices, pred_energy, 0.0))
    spread_ref[...] = jnp.broadcast_to(jnp.sum(energies, axis=0, keepdims=True), spread_ref.shape)
    kept_ref[...] = wave_ref[:, :KEPT]
    for copy in writes:
        copy.wait()


def subtract_kernel(total_ref, kept_ref, wave_ref, mult_ref, out_ref, held_ref, in_sems, out_sems):
    slices = wave_ref.shape[1]
    reads = {}
    for f in range(KEPT, slices):
        reads[f] = pltpu.make_async_copy(wave_ref.at[:, f], held_ref.at[:, f], in_sems.at[f])
        reads[f].start()
    sums = jnp.sum(total_ref[...], axis=0, keepdims=True)
    row = iota((1, LANES), 1)
    writes = []
    for f in range(slices):
        data = jnp.sum(jnp.where(row == f, sums, 0.0), axis=1, keepdims=True)
        pred = jnp.sum(jnp.where(row == slices + f, sums, 0.0), axis=1, keepdims=True)
        gain = jnp.sqrt((data + 1e-06) / (pred + 1e-06))
        if f in reads:
            reads[f].wait()
        source_ref = held_ref if f in reads else kept_ref
        for x in range(2):
            held_ref[x, f] = source_ref[x, f] - gain * mult_ref[x, f]
        writes.append(pltpu.make_async_copy(held_ref.at[:, f], out_ref.at[:, f], out_sems.at[f]))
        writes[-1].start()
    for copy in writes:
        copy.wait()


VMEM = pl.BlockSpec(memory_space=pltpu.VMEM)
SMEM = pl.BlockSpec(memory_space=pltpu.SMEM)
HBM = pl.BlockSpec(memory_space=pltpu.HBM)
ANY = pl.BlockSpec(memory_space=pl.ANY)


def on_chip(*arrays):
    return [pltpu.with_memory_space_constraint(a, pltpu.VMEM) for a in arrays]


def call(kernel, in_specs, out_shapes, flops, out_specs=None, scratch=(), aliases=None):
    return pl.pallas_call(
        kernel,
        in_specs=in_specs,
        out_specs=out_specs or [VMEM] * len(out_shapes),
        out_shape=out_shapes,
        scratch_shapes=list(scratch),
        input_output_aliases=aliases or {},
        cost_estimate=pl.CostEstimate(flops=flops, transcendentals=0, bytes_accessed=1 << 20),
        compiler_params=pltpu.CompilerParams(vmem_limit_bytes=24 << 20),
    )


def neighbours(axis):
    count = lax.axis_size(axis)
    up = [(i, i + 1) for i in range(count - 1)]
    return up, [(j, i) for i, j in up]


def swaps(axis, first):
    count = lax.axis_size(axis)
    pairs = [(i, i + 1) for i in range(first, count - 1, 2)]
    return pairs + [(j, i) for i, j in pairs]


def per_device(wavefield, surface_band, band_shift, trace_mask, shot_taper):
    _, slices, receivers, shots = wavefield.shape
    src_up, src_down = neighbours(SRC)
    mask = trace_mask.reshape(1, receivers)
    devices = lax.axis_size(SRC_RCV)
    in_hbm = pltpu.with_memory_space_constraint(wavefield, pltpu.HBM)

    wave, ends = call(
        head_kernel,
        [HBM, HBM],
        [pltpu.VMEM((2, slices, receivers, shots), F32), pltpu.VMEM((BLOCK, LANES), F32)],
        1 << 20,
        scratch=[pltpu.VMEM((1, receivers), jnp.int32), pltpu.SemaphoreType.DMA((3,))],
    )(in_hbm, pltpu.with_memory_space_constraint(mask, pltpu.HBM))
    after = lax.ppermute(ends, SRC, src_down)
    before = lax.ppermute(ends, SRC, src_up)

    wave, band = on_chip(wave, surface_band)
    head, link, chip = call(
        rest_kernel,
        [VMEM, VMEM],
        [
            pltpu.VMEM((2 * FIRST * HALO, shots), F32),
            pltpu.VMEM((2 * (slices - FIRST) * HALO + HALO // 2, shots), F32),
            pltpu.VMEM((2 * slices * HALO + HALO // 2, shots), F32),
        ],
        1 << 20,
    )(wave, mask)
    head = lax.ppermute(head, RCV, swaps(RCV, 1))

    before, after, link, chip = on_chip(before, after, link, chip)
    link, chip = call(
        pack_kernel,
        [VMEM, VMEM, ANY, ANY],
        [pltpu.VMEM(link.shape, F32), pltpu.VMEM(chip.shape, F32)],
        1 << 16,
        aliases={2: 0, 3: 1},
    )(before, after, link, chip)
    link = lax.ppermute(link, RCV, swaps(RCV, 1))
    chip = lax.ppermute(chip, RCV, swaps(RCV, 0))

    rows = 2 * receivers
    high, low, data_energy = call(
        band_kernel,
        [VMEM, VMEM],
        [
            pltpu.VMEM((slices, rows, 2 * LANES), BF16),
            pltpu.VMEM((slices, rows, 2 * LANES), BF16),
            pltpu.VMEM((slices, LANES), F32),
        ],
        1 << 28,
    )(wave, band)
    high, low, head, chip = on_chip(high, low, head, chip)
    frame = (2, shots // LANES, 2 * HALO + BLOCK, LANES)
    partial, taper_high, taper_low = call(
        gather_kernel,
        [SMEM, SMEM] + [VMEM] * 6,
        [
            pltpu.VMEM((FIRST, rows, shots), F32),
            pltpu.VMEM((shots, shots), BF16),
            pltpu.VMEM((shots, shots), BF16),
        ],
        1 << 28,
        scratch=[pltpu.VMEM((FIRST,) + frame, F32)] + [pltpu.VMEM((FIRST * rows, shots), BF16)] * 2,
    )(band_shift, shot_taper, wave, mask, high, low, head, chip)
    multiples, scaled, spread, kept = call(
        finish_kernel,
        [SMEM, SMEM] + [VMEM] * 12,
        [
            jax.ShapeDtypeStruct((2, slices, receivers, shots), F32),
            pltpu.VMEM((2, slices, receivers, shots), F32),
            pltpu.VMEM((devices, LANES), F32),
            pltpu.VMEM((2, KEPT, receivers, shots), F32),
        ],
        1 << 28,
        out_specs=[HBM, VMEM, VMEM, VMEM],
        scratch=[
            pltpu.VMEM((slices - FIRST + 1,) + frame, F32),
            pltpu.VMEM((slices - FIRST, rows, shots), F32),
            pltpu.SemaphoreType.DMA((slices // 4,)),
        ],
    )(
        band_shift, shot_taper, wave, mask, high, low, *on_chip(partial, taper_high, taper_low, link), chip, before,
        after, *on_chip(data_energy),
    )

    energies = lax.all_to_all(spread[:, None], SRC_RCV, 0, 0, tiled=True).reshape(devices, LANES)

    (primaries,) = call(
        subtract_kernel,
        [VMEM, VMEM, HBM, VMEM],
        [jax.ShapeDtypeStruct((2, slices, receivers, shots), F32)],
        1 << 20,
        out_specs=[HBM],
        scratch=[pltpu.VMEM((2, slices, receivers, shots), F32)] + [pltpu.SemaphoreType.DMA((slices,))] * 2,
    )(*on_chip(energies, kept), in_hbm, *on_chip(scaled))
    return (multiples, primaries)


def solution(mesh):
    split_mesh = Mesh(
        mesh.devices.reshape(4, 2, 2, 8, 2), ("src_0", "src_1", "rcv_0", "rcv_1", "rcv_2")
    )
    return jax.shard_map(
        per_device,
        mesh=split_mesh,
        in_specs=(P(None, None, RCV, SRC), P(None, RCV, None), P(RCV), P(RCV), P()),
        out_specs=(P(None, None, RCV, SRC), P(None, None, RCV, SRC)),
        check_vma=False,
    )
```

```python
import functools

import jax
import jax.numpy as jnp
from jax import lax
from jax.experimental import pallas as pl
from jax.experimental.pallas import tpu as pltpu
from jax.sharding import Mesh
from jax.sharding import PartitionSpec as P

APER = 64
SHIFT = 16
BLOCK = 64
SHALF = 2
HALO = APER // 2 + SHIFT
SPARE = BLOCK - HALO
LANES = 128
RCV = ("rcv_0", "rcv_1", "rcv_2")
SRC = ("src_0", "src_1")
SRC_RCV = ("src_0", "src_1", "rcv_0", "rcv_1", "rcv_2")
F32 = jnp.float32
BF16 = jnp.bfloat16
EARLY = 9
FIRST = 13
KEPT = 8


def iota(shape, dim):
    return lax.broadcasted_iota(jnp.int32, shape, dim)


def split(x):
    high = x.astype(BF16)
    return high, (x - high.astype(F32)).astype(BF16)


def product(a, b):
    dot = functools.partial(jnp.dot, preferred_element_type=F32)
    return dot(a[0], b[0]) + (dot(a[0], b[1]) + dot(a[1], b[0]))


def mask_column(mask_ref):
    row = jnp.broadcast_to(mask_ref[...].astype(F32), (BLOCK, BLOCK))
    diagonal = iota((BLOCK, BLOCK), 0) == iota((BLOCK, BLOCK), 1)
    return jnp.sum(jnp.where(diagonal, row, 0.0), axis=1, keepdims=True)


def is_odd():
    return lax.axis_index("rcv_2") == 1


def at_end(column, tail):
    return jnp.where(tail, column[SPARE:], column[:HALO])


def head_kernel(wave_ref, mask_ref, held_ref, early_ref, live_ref, sems):
    tail = is_odd()
    slices = wave_ref.shape[1]
    copies = [pltpu.make_async_copy(mask_ref, live_ref, sems.at[2])]
    for i, (low, high) in enumerate([(0, EARLY), (EARLY, slices)]):
        part = pl.ds(low, high - low)
        copies.append(pltpu.make_async_copy(wave_ref.at[:, part], held_ref.at[:, part], sems.at[i]))
    for copy in copies:
        copy.start()
    copies[0].wait()
    mask = at_end(mask_column(live_ref), tail)
    start = pl.multiple_of(jnp.where(tail, SPARE, 0), 8)
    copies[1].wait()
    for x in range(2):
        for f in range(EARLY):
            row = (2 * f + x) * HALO
            early_ref[row : row + HALO] = held_ref[x, f, pl.ds(start, HALO)] * mask
    copies[2].wait()


def rest_kernel(wave_ref, mask_ref, late_ref, link_ref, chip_ref, ends_ref):
    odd = is_odd()
    mask = mask_column(mask_ref)
    slices = wave_ref.shape[1]
    lane = iota((BLOCK, LANES), 1)
    ends = jnp.zeros((BLOCK, LANES), F32)
    for f in range(slices):
        for x in range(2):
            masked = wave_ref[x, f] * mask
            row = (2 * f + x) * HALO
            chip_ref[row : row + HALO] = at_end(masked, jnp.logical_not(odd))
            if f >= FIRST:
                row -= 2 * FIRST * HALO
                link_ref[row : row + HALO] = at_end(masked, odd)
            elif f >= EARLY:
                row -= 2 * EARLY * HALO
                late_ref[row : row + HALO] = at_end(masked, odd)
            place = 4 * (x * slices + f)
            last = pltpu.roll(masked[:, -LANES:], (place + SHALF) % LANES, 1)
            first = pltpu.roll(masked[:, :LANES], place + SHALF, 1)
            ends = jnp.where(lane // 2 == place // 2, last, ends)
            ends = jnp.where(lane // 2 == place // 2 + 1, first, ends)
    ends_ref[...] = ends


def merged_ends(before_ref, after_ref):
    return jnp.where(iota((BLOCK, LANES), 1) % 4 < SHALF, before_ref[...], after_ref[...])


def pack_kernel(before_ref, after_ref, _link_in, link_ref, ends_ref):
    odd = is_odd()
    ends = merged_ends(before_ref, after_ref)
    rows = at_end(ends, odd)
    link_ref[link_ref.shape[0] - HALO // 2 :] = jnp.concatenate([rows[: HALO // 2], rows[HALO // 2 :]], axis=1)
    ends_ref[...] = at_end(ends, jnp.logical_not(odd))


def band_kernel(taper_ref, wave_ref, band_ref, high_ref, low_ref, th_ref, tl_ref, energy_ref):
    shots = wave_ref.shape[3]
    th_ref[...], tl_ref[...] = split(weights_at(taper_ref, iota((shots, shots), 0) - iota((shots, shots), 1)))
    low_half = iota((BLOCK, LANES), 1) < APER
    for f in range(wave_ref.shape[1]):
        at = (f // 2) * LANES
        skewed = []
        for x in range(2):
            taps = jnp.where(low_half == (f % 2 == 0), band_ref[x, :, at : at + LANES], 0.0)
            skewed.append(pltpu.roll(taps, APER * (f % 2), 1, stride=1, stride_axis=0))
        real, imag = skewed
        for row, parts in enumerate([(real, -imag), (imag, real)]):
            for column, part in enumerate(parts):
                place = (f, slice(row * BLOCK, (row + 1) * BLOCK), slice(column * LANES, (column + 1) * LANES))
                high_ref[place], low_ref[place] = split(part)
        squares = wave_ref[0, f] * wave_ref[0, f] + wave_ref[1, f] * wave_ref[1, f]
        squares = jnp.sum(squares, axis=0, keepdims=True)
        energy_ref[f : f + 1, :] = squares[:, :LANES] + squares[:, LANES:]


def framed(frame_ref, own, chip, link, start):
    odd = is_odd()
    left, right = 0, HALO + BLOCK
    frame_ref[HALO : HALO + BLOCK] = own
    frame_ref[pl.ds(pl.multiple_of(jnp.where(odd, left, right), 8), HALO)] = chip
    frame_ref[pl.ds(pl.multiple_of(jnp.where(odd, right, left), 8), HALO)] = link
    return frame_ref[pl.ds(start, LANES)]


def window(frames_ref, wave_ref, mask, chip_ref, link, f, start):
    rows = []
    for x in range(2):
        own = wave_ref[x, f] * mask
        at = (2 * f + x) * HALO
        chip = chip_ref[at : at + HALO]
        other = link(x)
        columns = []
        for tile in range(own.shape[1] // LANES):
            part = slice(tile * LANES, (tile + 1) * LANES)
            columns.append(framed(frames_ref.at[x, tile], own[:, part], chip[:, part], other[:, part], start))
        rows.append(jnp.concatenate(columns, axis=1))
    return jnp.concatenate(rows, axis=0)


def gather_kernel(
    base, shift_ref, wave_ref, mask_ref, high_ref, low_ref, th_ref, tl_ref, link_ref, chip_ref, part_ref, frames_ref,
    ph_ref, pl_ref,
):
    start = SPARE + shift_ref[0]
    mask = mask_column(mask_ref)
    count, rows, shots = part_ref.shape

    def linked(x, i):
        at = (2 * i + x) * HALO
        return link_ref[at : at + HALO]

    for i in range(count):
        f = base + i
        data = window(frames_ref.at[i], wave_ref, mask, chip_ref, lambda x, i=i: linked(x, i), f, start)
        ph_ref[i * rows : (i + 1) * rows], pl_ref[i * rows : (i + 1) * rows] = split(
            product((high_ref[f], low_ref[f]), split(data))
        )
    whole = product((ph_ref[...], pl_ref[...]), (th_ref[...], tl_ref[...]))
    part_ref[...] = whole.reshape(count, rows, shots)


def weights_at(taper_ref, ahead):
    weights = jnp.zeros(ahead.shape, F32)
    for u in range(2 * SHALF + 1):
        weights = jnp.where(ahead == u - SHALF, taper_ref[u], weights)
    return weights


def finish_kernel(
    shift_ref, taper_ref, wave_ref, mask_ref, high_ref, low_ref, th_ref, tl_ref, early_ref, late_ref, link_ref, chip_ref,
    ends_ref, before_ref, after_ref, data_ref, mult_ref, sums_ref, kept_ref, frames_ref, pred_ref,
):
    start = SPARE + shift_ref[0]
    slices = wave_ref.shape[1]
    shots = wave_ref.shape[3]
    rows = 2 * BLOCK
    mask = mask_column(mask_ref)

    def linked(x, f):
        at = (2 * (f - FIRST) + x) * HALO
        return link_ref[at : at + HALO]

    packed = link_ref[link_ref.shape[0] - HALO // 2 :]
    packed = jnp.concatenate([packed[:, :LANES], packed[:, LANES:]], axis=0)
    ends = framed(
        frames_ref.at[slices - FIRST, 0, 0], merged_ends(before_ref, after_ref), ends_ref[...], packed, start
    )
    ends = split(ends)
    kind = iota((LANES, LANES), 0) % 4
    source = jnp.where(kind < SHALF, kind - SHALF, kind - SHALF + shots)
    target = iota((LANES, LANES), 1)
    target = jnp.where(target < LANES // 2, target, target + shots - LANES)
    reach = split(weights_at(taper_ref, source - target))
    for f in range(FIRST, slices):
        data = window(frames_ref.at[f - FIRST], wave_ref, mask, chip_ref, lambda x, f=f: linked(x, f), f, start)
        pred = split(product((high_ref[f], low_ref[f]), split(data)))
        pred_ref[f - FIRST] = product(pred, (th_ref[...], tl_ref[...]))
    near = iota((rows, LANES), 1) < LANES // 2
    squares = []
    group = 4
    for first in range(0, slices, group):
        shape = (group, rows, LANES)
        owner = iota(shape, 2) // 4 - iota(shape, 0) - first
        edge = jnp.zeros(shape, F32)
        for x in range(2):
            part = slice(x * LANES, (x + 1) * LANES)
            matrices = tuple(ref[first : first + group, :, part].reshape(group * rows, LANES) for ref in (high_ref, low_ref))
            edge = jnp.where(owner == x * slices, product(matrices, ends).reshape(shape), edge)
        edge = product(split(edge.reshape(group * rows, LANES)), reach)
        for f in range(first, first + group):
            own = early_ref[f] if f < EARLY else late_ref[f - EARLY] if f < FIRST else pred_ref[f - FIRST]
            extra = edge[(f - first) * rows : (f - first + 1) * rows]
            total = jnp.concatenate(
                [own[:, :LANES] + jnp.where(near, extra, 0.0), own[:, LANES:] + jnp.where(near, 0.0, extra)], axis=1
            )
            mult_ref[0, f] = total[:BLOCK]
            mult_ref[1, f] = total[BLOCK:]
            total = jnp.sum(total * total, axis=0, keepdims=True)
            squares.append(total[:, :LANES] + total[:, LANES:])
    lane = iota((slices, LANES), 1) - iota((slices, LANES), 0)
    row = iota((slices, LANES), 0)
    pred_rows = jnp.zeros((slices, LANES), F32)
    for f in range(slices):
        pred_rows = jnp.where(row == f, squares[f], pred_rows)
    pred_energy = jnp.sum(pred_rows, axis=1, keepdims=True)
    data_energy = jnp.sum(data_ref[...], axis=1, keepdims=True)
    energies = jnp.where(lane == 0, data_energy, jnp.where(lane == slices, pred_energy, 0.0))
    sums_ref[...] = jnp.sum(energies, axis=0, keepdims=True)
    kept_ref[...] = wave_ref[:, :KEPT]


def subtract_kernel(total_ref, kept_ref, wave_ref, mult_ref, out_ref, held_ref, in_sems, out_sems):
    slices = wave_ref.shape[1]
    reads = {}
    for f in range(KEPT, slices):
        reads[f] = pltpu.make_async_copy(wave_ref.at[:, f], held_ref.at[:, f], in_sems.at[f])
        reads[f].start()
    sums = jnp.sum(total_ref[...], axis=0, keepdims=True)
    row = iota((1, LANES), 1)
    writes = []
    for f in range(slices):
        data = jnp.sum(jnp.where(row == f, sums, 0.0), axis=1, keepdims=True)
        pred = jnp.sum(jnp.where(row == slices + f, sums, 0.0), axis=1, keepdims=True)
        gain = jnp.sqrt((data + 1e-06) / (pred + 1e-06))
        if f in reads:
            reads[f].wait()
        source_ref = held_ref if f in reads else kept_ref
        for x in range(2):
            held_ref[x, f] = source_ref[x, f] - gain * mult_ref[x, f]
        writes.append(pltpu.make_async_copy(held_ref.at[:, f], out_ref.at[:, f], out_sems.at[f]))
        writes[-1].start()
    for copy in writes:
        copy.wait()


VMEM = pl.BlockSpec(memory_space=pltpu.VMEM)
SMEM = pl.BlockSpec(memory_space=pltpu.SMEM)
HBM = pl.BlockSpec(memory_space=pltpu.HBM)
ANY = pl.BlockSpec(memory_space=pl.ANY)


def on_chip(*arrays):
    return [pltpu.with_memory_space_constraint(a, pltpu.VMEM) for a in arrays]


def call(kernel, in_specs, out_shapes, flops, out_specs=None, scratch=(), aliases=None):
    return pl.pallas_call(
        kernel,
        in_specs=in_specs,
        out_specs=out_specs or [VMEM] * len(out_shapes),
        out_shape=out_shapes,
        scratch_shapes=list(scratch),
        input_output_aliases=aliases or {},
        cost_estimate=pl.CostEstimate(flops=flops, transcendentals=0, bytes_accessed=1 << 20),
        compiler_params=pltpu.CompilerParams(vmem_limit_bytes=24 << 20),
    )


def neighbours(axis):
    count = lax.axis_size(axis)
    up = [(i, i + 1) for i in range(count - 1)]
    return up, [(j, i) for i, j in up]


def swaps(axis, first):
    count = lax.axis_size(axis)
    pairs = [(i, i + 1) for i in range(first, count - 1, 2)]
    return pairs + [(j, i) for i, j in pairs]


def per_device(wavefield, surface_band, band_shift, trace_mask, shot_taper):
    _, slices, receivers, shots = wavefield.shape
    src_up, src_down = neighbours(SRC)
    mask = trace_mask.reshape(1, receivers)
    devices = lax.axis_size(SRC_RCV)
    in_hbm = pltpu.with_memory_space_constraint(wavefield, pltpu.HBM)

    rows = 2 * receivers

    def in_vmem(*shape, dtype=F32):
        return pltpu.VMEM(shape, dtype)

    wave, early = call(
        head_kernel,
        [HBM, HBM],
        [in_vmem(2, slices, receivers, shots), in_vmem(2 * EARLY * HALO, shots)],
        1 << 20,
        scratch=[pltpu.VMEM((1, receivers), jnp.int32), pltpu.SemaphoreType.DMA((3,))],
    )(in_hbm, pltpu.with_memory_space_constraint(mask, pltpu.HBM))
    early = lax.ppermute(early, RCV, swaps(RCV, 1))

    wave, band = on_chip(wave, surface_band)
    late, link, chip, ends = call(
        rest_kernel,
        [VMEM, VMEM],
        [
            in_vmem(2 * (FIRST - EARLY) * HALO, shots),
            in_vmem(2 * (slices - FIRST) * HALO + HALO // 2, shots),
            in_vmem(2 * slices * HALO, shots),
            in_vmem(BLOCK, LANES),
        ],
        1 << 20,
    )(wave, mask)
    after = lax.ppermute(ends, SRC, src_down)
    before = lax.ppermute(ends, SRC, src_up)
    late = lax.ppermute(late, RCV, swaps(RCV, 1))

    chip = lax.ppermute(chip, RCV, swaps(RCV, 0))

    before, after, link = on_chip(before, after, link)
    link, ends = call(
        pack_kernel, [VMEM, VMEM, ANY], [in_vmem(*link.shape), in_vmem(HALO, LANES)], 1 << 16, aliases={2: 0}
    )(before, after, link)
    link = lax.ppermute(link, RCV, swaps(RCV, 1))
    ends = lax.ppermute(ends, RCV, swaps(RCV, 0))

    high, low, taper_high, taper_low, data_energy = call(
        band_kernel,
        [SMEM, VMEM, VMEM],
        [
            in_vmem(slices, rows, 2 * LANES, dtype=BF16),
            in_vmem(slices, rows, 2 * LANES, dtype=BF16),
            in_vmem(shots, shots, dtype=BF16),
            in_vmem(shots, shots, dtype=BF16),
            in_vmem(slices, LANES),
        ],
        1 << 28,
    )(shot_taper, wave, band)
    matrices = on_chip(high, low, taper_high, taper_low)
    early, late, link, chip, ends = on_chip(early, late, link, chip, ends)
    frame = (2, shots // LANES, 2 * HALO + BLOCK, LANES)

    def gathered(base, count, message):
        (part,) = call(
            functools.partial(gather_kernel, base),
            [SMEM] + [VMEM] * 8,
            [in_vmem(count, rows, shots)],
            1 << 28,
            scratch=[pltpu.VMEM((count,) + frame, F32)] + [pltpu.VMEM((count * rows, shots), BF16)] * 2,
        )(band_shift, wave, mask, *matrices, message, chip)
        return part

    parts = on_chip(gathered(0, EARLY, early), gathered(EARLY, FIRST - EARLY, late))
    multiples, sums, kept = call(
        finish_kernel,
        [SMEM, SMEM] + [VMEM] * 14,
        [in_vmem(2, slices, receivers, shots), in_vmem(1, LANES), in_vmem(2, KEPT, receivers, shots)],
        1 << 28,
        scratch=[
            pltpu.VMEM((slices - FIRST + 1,) + frame, F32),
            pltpu.VMEM((slices - FIRST, rows, shots), F32),
        ],
    )(
        band_shift, shot_taper, wave, mask, *matrices, *parts, link, chip, ends, before, after, *on_chip(data_energy),
    )

    spread = jnp.broadcast_to(sums[None], (devices, 1, LANES))
    energies = lax.all_to_all(spread, SRC_RCV, 0, 0, tiled=True).reshape(devices, LANES)

    (primaries,) = call(
        subtract_kernel,
        [VMEM, VMEM, HBM, VMEM],
        [jax.ShapeDtypeStruct((2, slices, receivers, shots), F32)],
        1 << 20,
        out_specs=[HBM],
        scratch=[pltpu.VMEM((2, slices, receivers, shots), F32)] + [pltpu.SemaphoreType.DMA((slices,))] * 2,
    )(*on_chip(energies, kept), in_hbm, *on_chip(multiples))
    return (multiples, primaries)


def solution(mesh):
    split_mesh = Mesh(
        mesh.devices.reshape(4, 2, 2, 8, 2), ("src_0", "src_1", "rcv_0", "rcv_1", "rcv_2")
    )
    return jax.shard_map(
        per_device,
        mesh=split_mesh,
        in_specs=(P(None, None, RCV, SRC), P(None, RCV, None), P(RCV), P(RCV), P()),
        out_specs=(P(None, None, RCV, SRC), P(None, None, RCV, SRC)),
        check_vma=False,
    )
```

```python
import functools

import jax
import jax.numpy as jnp
from jax import lax
from jax.experimental import pallas as pl
from jax.experimental.pallas import tpu as pltpu
from jax.sharding import Mesh
from jax.sharding import PartitionSpec as P

APER = 64
SHIFT = 16
BLOCK = 64
SHALF = 2
HALO = APER // 2 + SHIFT
SPARE = BLOCK - HALO
LANES = 128
RCV = ("rcv_0", "rcv_1", "rcv_2")
SRC = ("src_0", "src_1")
SRC_RCV = ("src_0", "src_1", "rcv_0", "rcv_1", "rcv_2")
F32 = jnp.float32
BF16 = jnp.bfloat16
EARLY = 9
FIRST = 13
KEPT = 8


def iota(shape, dim):
    return lax.broadcasted_iota(jnp.int32, shape, dim)


def split(x):
    high = x.astype(BF16)
    return high, (x - high.astype(F32)).astype(BF16)


def product(a, b):
    dot = functools.partial(jnp.dot, preferred_element_type=F32)
    return dot(a[0], b[0]) + (dot(a[0], b[1]) + dot(a[1], b[0]))


def mask_column(mask_ref):
    row = jnp.broadcast_to(mask_ref[...].astype(F32), (BLOCK, BLOCK))
    diagonal = iota((BLOCK, BLOCK), 0) == iota((BLOCK, BLOCK), 1)
    return jnp.sum(jnp.where(diagonal, row, 0.0), axis=1, keepdims=True)


def is_odd():
    return lax.axis_index("rcv_2") == 1


def at_end(column, tail):
    return jnp.where(tail, column[SPARE:], column[:HALO])


def head_kernel(wave_ref, mask_ref, held_ref, early_ref, live_ref, sems):
    tail = is_odd()
    slices = wave_ref.shape[1]
    copies = [pltpu.make_async_copy(mask_ref, live_ref, sems.at[2])]
    for i, (low, high) in enumerate([(0, EARLY), (EARLY, slices)]):
        part = pl.ds(low, high - low)
        copies.append(pltpu.make_async_copy(wave_ref.at[:, part], held_ref.at[:, part], sems.at[i]))
    for copy in copies:
        copy.start()
    copies[0].wait()
    mask = at_end(mask_column(live_ref), tail)
    start = pl.multiple_of(jnp.where(tail, SPARE, 0), 8)
    copies[1].wait()
    for x in range(2):
        for f in range(EARLY):
            row = (2 * f + x) * HALO
            early_ref[row : row + HALO] = held_ref[x, f, pl.ds(start, HALO)] * mask
    copies[2].wait()


def rest_kernel(wave_ref, mask_ref, late_ref, link_ref, chip_ref, ends_ref):
    odd = is_odd()
    mask = mask_column(mask_ref)
    slices = wave_ref.shape[1]
    lane = iota((BLOCK, LANES), 1)
    ends = jnp.zeros((BLOCK, LANES), F32)
    for f in range(slices):
        for x in range(2):
            masked = wave_ref[x, f] * mask
            row = (2 * f + x) * HALO
            chip_ref[row : row + HALO] = at_end(masked, jnp.logical_not(odd))
            if f >= FIRST:
                row -= 2 * FIRST * HALO
                link_ref[row : row + HALO] = at_end(masked, odd)
            elif f >= EARLY:
                row -= 2 * EARLY * HALO
                late_ref[row : row + HALO] = at_end(masked, odd)
            place = 4 * (x * slices + f)
            last = pltpu.roll(masked[:, -LANES:], (place + SHALF) % LANES, 1)
            first = pltpu.roll(masked[:, :LANES], place + SHALF, 1)
            ends = jnp.where(lane // 2 == place // 2, last, ends)
            ends = jnp.where(lane // 2 == place // 2 + 1, first, ends)
    ends_ref[...] = ends


def merged_ends(before_ref, after_ref):
    return jnp.where(iota((BLOCK, LANES), 1) % 4 < SHALF, before_ref[...], after_ref[...])


def pack_kernel(before_ref, after_ref, _link_in, link_ref, ends_ref):
    odd = is_odd()
    ends = merged_ends(before_ref, after_ref)
    rows = at_end(ends, odd)
    link_ref[link_ref.shape[0] - HALO // 2 :] = jnp.concatenate([rows[: HALO // 2], rows[HALO // 2 :]], axis=1)
    ends_ref[...] = at_end(ends, jnp.logical_not(odd))


def band_kernel(taper_ref, wave_ref, band_ref, high_ref, low_ref, th_ref, tl_ref, energy_ref):
    shots = wave_ref.shape[3]
    th_ref[...], tl_ref[...] = split(weights_at(taper_ref, iota((shots, shots), 0) - iota((shots, shots), 1)))
    low_half = iota((BLOCK, LANES), 1) < APER
    for f in range(wave_ref.shape[1]):
        at = (f // 2) * LANES
        skewed = []
        for x in range(2):
            taps = jnp.where(low_half == (f % 2 == 0), band_ref[x, :, at : at + LANES], 0.0)
            skewed.append(pltpu.roll(taps, APER * (f % 2), 1, stride=1, stride_axis=0))
        real, imag = skewed
        for row, parts in enumerate([(real, -imag), (imag, real)]):
            for column, part in enumerate(parts):
                place = (f, slice(row * BLOCK, (row + 1) * BLOCK), slice(column * LANES, (column + 1) * LANES))
                high_ref[place], low_ref[place] = split(part)
        squares = wave_ref[0, f] * wave_ref[0, f] + wave_ref[1, f] * wave_ref[1, f]
        squares = jnp.sum(squares, axis=0, keepdims=True)
        energy_ref[f : f + 1, :] = squares[:, :LANES] + squares[:, LANES:]


def framed(frame_ref, own, chip, link, start):
    odd = is_odd()
    left, right = 0, HALO + BLOCK
    frame_ref[HALO : HALO + BLOCK] = own
    frame_ref[pl.ds(pl.multiple_of(jnp.where(odd, left, right), 8), HALO)] = chip
    frame_ref[pl.ds(pl.multiple_of(jnp.where(odd, right, left), 8), HALO)] = link
    return frame_ref[pl.ds(start, LANES)]


def window(frames_ref, wave_ref, mask, chip_ref, link, f, start):
    rows = []
    for x in range(2):
        own = wave_ref[x, f] * mask
        at = (2 * f + x) * HALO
        chip = chip_ref[at : at + HALO]
        other = link(x)
        columns = []
        for tile in range(own.shape[1] // LANES):
            part = slice(tile * LANES, (tile + 1) * LANES)
            columns.append(framed(frames_ref.at[x, tile], own[:, part], chip[:, part], other[:, part], start))
        rows.append(jnp.concatenate(columns, axis=1))
    return jnp.concatenate(rows, axis=0)


def gather_kernel(
    base, shift_ref, wave_ref, mask_ref, high_ref, low_ref, th_ref, tl_ref, link_ref, chip_ref, part_ref, frames_ref,
    ph_ref, pl_ref,
):
    start = SPARE + shift_ref[0]
    mask = mask_column(mask_ref)
    count, rows, shots = part_ref.shape

    def linked(x, i):
        at = (2 * i + x) * HALO
        return link_ref[at : at + HALO]

    for i in range(count):
        f = base + i
        data = window(frames_ref.at[i], wave_ref, mask, chip_ref, lambda x, i=i: linked(x, i), f, start)
        ph_ref[i * rows : (i + 1) * rows], pl_ref[i * rows : (i + 1) * rows] = split(
            product((high_ref[f], low_ref[f]), split(data))
        )
    whole = product((ph_ref[...], pl_ref[...]), (th_ref[...], tl_ref[...]))
    part_ref[...] = whole.reshape(count, rows, shots)


def weights_at(taper_ref, ahead):
    weights = jnp.zeros(ahead.shape, F32)
    for u in range(2 * SHALF + 1):
        weights = jnp.where(ahead == u - SHALF, taper_ref[u], weights)
    return weights


def stored(mult_ref, squares_ref, f, own, extra):
    near = iota(extra.shape, 1) < LANES // 2
    total = jnp.concatenate(
        [own[:, :LANES] + jnp.where(near, extra, 0.0), own[:, LANES:] + jnp.where(near, 0.0, extra)], axis=1
    )
    mult_ref[0, f] = total[:BLOCK]
    mult_ref[1, f] = total[BLOCK:]
    total = jnp.sum(total * total, axis=0, keepdims=True)
    squares_ref[f : f + 1, :] = total[:, :LANES] + total[:, LANES:]


def merge_kernel(
    shift_ref, taper_ref, wave_ref, mask_ref, high_ref, low_ref, th_ref, tl_ref, early_ref, late_ref, chip_ref, ends_ref,
    before_ref, after_ref, mult_ref, edge_ref, squares_ref, kept_ref, frames_ref, ph_ref, pl_ref, part_ref,
):
    start = SPARE + shift_ref[0]
    slices = wave_ref.shape[1]
    shots = wave_ref.shape[3]
    rows = 2 * BLOCK
    count = FIRST - EARLY
    packed = late_ref[late_ref.shape[0] - HALO // 2 :]
    packed = jnp.concatenate([packed[:, :LANES], packed[:, LANES:]], axis=0)
    ends = split(
        framed(frames_ref.at[count, 0, 0], merged_ends(before_ref, after_ref), ends_ref[...], packed, start)
    )
    kind = iota((LANES, LANES), 0) % 4
    source = jnp.where(kind < SHALF, kind - SHALF, kind - SHALF + shots)
    target = iota((LANES, LANES), 1)
    target = jnp.where(target < LANES // 2, target, target + shots - LANES)
    reach = split(weights_at(taper_ref, source - target))
    gather_kernel(
        EARLY, shift_ref, wave_ref, mask_ref, high_ref, low_ref, th_ref, tl_ref, late_ref, chip_ref, part_ref, frames_ref,
        ph_ref, pl_ref,
    )
    kept_ref[...] = wave_ref[:, :KEPT]
    group = 4
    for first in range(0, slices, group):
        shape = (group, rows, LANES)
        owner = iota(shape, 2) // 4 - iota(shape, 0) - first
        edge = jnp.zeros(shape, F32)
        for x in range(2):
            part = slice(x * LANES, (x + 1) * LANES)
            matrices = tuple(ref[first : first + group, :, part].reshape(group * rows, LANES) for ref in (high_ref, low_ref))
            edge = jnp.where(owner == x * slices, product(matrices, ends).reshape(shape), edge)
        edge = product(split(edge.reshape(group * rows, LANES)), reach)
        for f in range(first, first + group):
            extra = edge[(f - first) * rows : (f - first + 1) * rows]
            if f >= FIRST:
                edge_ref[f - FIRST] = extra
            else:
                stored(mult_ref, squares_ref, f, early_ref[f] if f < EARLY else part_ref[f - EARLY], extra)
    squares_ref[FIRST:] = jnp.zeros((slices - FIRST, LANES), F32)


def finish_kernel(
    shift_ref, wave_ref, mask_ref, high_ref, low_ref, th_ref, tl_ref, link_ref, chip_ref, edge_ref, some_ref, data_ref,
    _mult_in, mult_ref, sums_ref, frames_ref, ph_ref, pl_ref, part_ref, squares_ref,
):
    slices = wave_ref.shape[1]
    gather_kernel(
        FIRST, shift_ref, wave_ref, mask_ref, high_ref, low_ref, th_ref, tl_ref, link_ref, chip_ref, part_ref, frames_ref,
        ph_ref, pl_ref,
    )
    squares_ref[...] = some_ref[...]
    for f in range(FIRST, slices):
        stored(mult_ref, squares_ref, f, part_ref[f - FIRST], edge_ref[f - FIRST])
    pred_energy = jnp.sum(squares_ref[...], axis=1, keepdims=True)
    data_energy = jnp.sum(data_ref[...], axis=1, keepdims=True)
    place = iota((slices, LANES), 1) - iota((slices, LANES), 0)
    energies = jnp.where(place == 0, data_energy, jnp.where(place == slices, pred_energy, 0.0))
    sums_ref[...] = jnp.sum(energies, axis=0, keepdims=True)


def subtract_kernel(total_ref, kept_ref, wave_ref, mult_ref, out_ref, held_ref, in_sems, out_sems):
    slices = wave_ref.shape[1]
    reads = {}
    for f in range(KEPT, slices):
        reads[f] = pltpu.make_async_copy(wave_ref.at[:, f], held_ref.at[:, f], in_sems.at[f])
        reads[f].start()
    sums = jnp.sum(total_ref[...], axis=0, keepdims=True)
    row = iota((1, LANES), 1)
    writes = []
    for f in range(slices):
        data = jnp.sum(jnp.where(row == f, sums, 0.0), axis=1, keepdims=True)
        pred = jnp.sum(jnp.where(row == slices + f, sums, 0.0), axis=1, keepdims=True)
        gain = jnp.sqrt((data + 1e-06) / (pred + 1e-06))
        if f in reads:
            reads[f].wait()
        source_ref = held_ref if f in reads else kept_ref
        for x in range(2):
            held_ref[x, f] = source_ref[x, f] - gain * mult_ref[x, f]
        writes.append(pltpu.make_async_copy(held_ref.at[:, f], out_ref.at[:, f], out_sems.at[f]))
        writes[-1].start()
    for copy in writes:
        copy.wait()


VMEM = pl.BlockSpec(memory_space=pltpu.VMEM)
SMEM = pl.BlockSpec(memory_space=pltpu.SMEM)
HBM = pl.BlockSpec(memory_space=pltpu.HBM)
ANY = pl.BlockSpec(memory_space=pl.ANY)


def on_chip(*arrays):
    return [pltpu.with_memory_space_constraint(a, pltpu.VMEM) for a in arrays]


def call(kernel, in_specs, out_shapes, flops, out_specs=None, scratch=(), aliases=None):
    return pl.pallas_call(
        kernel,
        in_specs=in_specs,
        out_specs=out_specs or [VMEM] * len(out_shapes),
        out_shape=out_shapes,
        scratch_shapes=list(scratch),
        input_output_aliases=aliases or {},
        cost_estimate=pl.CostEstimate(flops=flops, transcendentals=0, bytes_accessed=1 << 20),
        compiler_params=pltpu.CompilerParams(vmem_limit_bytes=24 << 20),
    )


def neighbours(axis):
    count = lax.axis_size(axis)
    up = [(i, i + 1) for i in range(count - 1)]
    return up, [(j, i) for i, j in up]


def swaps(axis, first):
    count = lax.axis_size(axis)
    pairs = [(i, i + 1) for i in range(first, count - 1, 2)]
    return pairs + [(j, i) for i, j in pairs]


def per_device(wavefield, surface_band, band_shift, trace_mask, shot_taper):
    _, slices, receivers, shots = wavefield.shape
    src_up, src_down = neighbours(SRC)
    mask = trace_mask.reshape(1, receivers)
    devices = lax.axis_size(SRC_RCV)
    in_hbm = pltpu.with_memory_space_constraint(wavefield, pltpu.HBM)

    rows = 2 * receivers

    def in_vmem(*shape, dtype=F32):
        return pltpu.VMEM(shape, dtype)

    wave, early = call(
        head_kernel,
        [HBM, HBM],
        [in_vmem(2, slices, receivers, shots), in_vmem(2 * EARLY * HALO, shots)],
        1 << 20,
        scratch=[pltpu.VMEM((1, receivers), jnp.int32), pltpu.SemaphoreType.DMA((3,))],
    )(in_hbm, pltpu.with_memory_space_constraint(mask, pltpu.HBM))
    early = lax.ppermute(early, RCV, swaps(RCV, 1))

    wave, band = on_chip(wave, surface_band)
    late, link, chip, ends = call(
        rest_kernel,
        [VMEM, VMEM],
        [
            in_vmem(2 * (FIRST - EARLY) * HALO + HALO // 2, shots),
            in_vmem(2 * (slices - FIRST) * HALO, shots),
            in_vmem(2 * slices * HALO, shots),
            in_vmem(BLOCK, LANES),
        ],
        1 << 20,
    )(wave, mask)
    after = lax.ppermute(ends, SRC, src_down)
    before = lax.ppermute(ends, SRC, src_up)
    chip = lax.ppermute(chip, RCV, swaps(RCV, 0))

    high, low, taper_high, taper_low, data_energy = call(
        band_kernel,
        [SMEM, VMEM, VMEM],
        [
            in_vmem(slices, rows, 2 * LANES, dtype=BF16),
            in_vmem(slices, rows, 2 * LANES, dtype=BF16),
            in_vmem(shots, shots, dtype=BF16),
            in_vmem(shots, shots, dtype=BF16),
            in_vmem(slices, LANES),
        ],
        1 << 28,
    )(shot_taper, wave, band)

    before, after, late = on_chip(before, after, late)
    late, ends = call(
        pack_kernel, [VMEM, VMEM, ANY], [in_vmem(*late.shape), in_vmem(HALO, LANES)], 1 << 16, aliases={2: 0}
    )(before, after, late)
    late = lax.ppermute(late, RCV, swaps(RCV, 1))
    link = lax.ppermute(link, RCV, swaps(RCV, 1))
    ends = lax.ppermute(ends, RCV, swaps(RCV, 0))

    matrices = on_chip(high, low, taper_high, taper_low)
    early, late, link, chip, ends = on_chip(early, late, link, chip, ends)
    frame = (2, shots // LANES, 2 * HALO + BLOCK, LANES)

    def workspace(count, frames):
        return [pltpu.VMEM((frames,) + frame, F32)] + [pltpu.VMEM((count * rows, shots), BF16)] * 2

    (part,) = call(
        functools.partial(gather_kernel, 0),
        [SMEM] + [VMEM] * 8,
        [in_vmem(EARLY, rows, shots)],
        1 << 28,
        scratch=workspace(EARLY, EARLY),
    )(band_shift, wave, mask, *matrices, early, chip)
    middle, last = FIRST - EARLY, slices - FIRST
    multiples, edge, squares, kept = call(
        merge_kernel,
        [SMEM, SMEM] + [VMEM] * 12,
        [
            in_vmem(2, slices, receivers, shots),
            in_vmem(last, rows, LANES),
            in_vmem(slices, LANES),
            in_vmem(2, KEPT, receivers, shots),
        ],
        1 << 28,
        scratch=workspace(middle, middle + 1) + [pltpu.VMEM((middle, rows, shots), F32)],
    )(band_shift, shot_taper, wave, mask, *matrices, *on_chip(part), late, chip, ends, before, after)
    multiples, sums = call(
        finish_kernel,
        [SMEM] + [VMEM] * 11 + [ANY],
        [in_vmem(2, slices, receivers, shots), in_vmem(1, LANES)],
        1 << 28,
        scratch=workspace(last, last) + [pltpu.VMEM((last, rows, shots), F32), pltpu.VMEM((slices, LANES), F32)],
        aliases={12: 0},
    )(band_shift, wave, mask, *matrices, link, chip, *on_chip(edge, squares, data_energy, multiples))

    spread = jnp.broadcast_to(sums[None], (devices, 1, LANES))
    energies = lax.all_to_all(spread, SRC_RCV, 0, 0, tiled=True).reshape(devices, LANES)

    (primaries,) = call(
        subtract_kernel,
        [VMEM, VMEM, HBM, VMEM],
        [jax.ShapeDtypeStruct((2, slices, receivers, shots), F32)],
        1 << 20,
        out_specs=[HBM],
        scratch=[pltpu.VMEM((2, slices, receivers, shots), F32)] + [pltpu.SemaphoreType.DMA((slices,))] * 2,
    )(*on_chip(energies, kept), in_hbm, *on_chip(multiples))
    return (multiples, primaries)


def solution(mesh):
    split_mesh = Mesh(
        mesh.devices.reshape(4, 2, 2, 8, 2), ("src_0", "src_1", "rcv_0", "rcv_1", "rcv_2")
    )
    return jax.shard_map(
        per_device,
        mesh=split_mesh,
        in_specs=(P(None, None, RCV, SRC), P(None, RCV, None), P(RCV), P(RCV), P()),
        out_specs=(P(None, None, RCV, SRC), P(None, None, RCV, SRC)),
        check_vma=False,
    )
```

```python
import functools

import jax
import jax.numpy as jnp
from jax import lax
from jax.experimental import pallas as pl
from jax.experimental.pallas import tpu as pltpu
from jax.sharding import Mesh
from jax.sharding import PartitionSpec as P

APER = 64
SHIFT = 16
BLOCK = 64
SHALF = 2
HALO = APER // 2 + SHIFT
SPARE = BLOCK - HALO
LANES = 128
RCV = ("rcv_0", "rcv_1", "rcv_2")
SRC = ("src_0", "src_1")
SRC_RCV = ("src_0", "src_1", "rcv_0", "rcv_1", "rcv_2")
F32 = jnp.float32
BF16 = jnp.bfloat16
EARLY = 9
FIRST = 13
KEPT = 9


def iota(shape, dim):
    return lax.broadcasted_iota(jnp.int32, shape, dim)


def split(x):
    high = x.astype(BF16)
    return high, (x - high.astype(F32)).astype(BF16)


def product(a, b):
    dot = functools.partial(jnp.dot, preferred_element_type=F32)
    return dot(a[0], b[0]) + (dot(a[0], b[1]) + dot(a[1], b[0]))


def mask_column(mask_ref):
    row = jnp.broadcast_to(mask_ref[...].astype(F32), (BLOCK, BLOCK))
    diagonal = iota((BLOCK, BLOCK), 0) == iota((BLOCK, BLOCK), 1)
    return jnp.sum(jnp.where(diagonal, row, 0.0), axis=1, keepdims=True)


def is_odd():
    return lax.axis_index("rcv_2") == 1


def at_end(column, tail):
    return jnp.where(tail, column[SPARE:], column[:HALO])


def head_kernel(wave_ref, mask_ref, held_ref, early_ref, live_ref, sems):
    tail = is_odd()
    slices = wave_ref.shape[1]
    copies = [pltpu.make_async_copy(mask_ref, live_ref, sems.at[2])]
    for i, (low, high) in enumerate([(0, EARLY), (EARLY, slices)]):
        part = pl.ds(low, high - low)
        copies.append(pltpu.make_async_copy(wave_ref.at[:, part], held_ref.at[:, part], sems.at[i]))
    for copy in copies:
        copy.start()
    copies[0].wait()
    mask = at_end(mask_column(live_ref), tail)
    start = pl.multiple_of(jnp.where(tail, SPARE, 0), 8)
    copies[1].wait()
    for x in range(2):
        for f in range(EARLY):
            row = (2 * f + x) * HALO
            early_ref[row : row + HALO] = held_ref[x, f, pl.ds(start, HALO)] * mask
    copies[2].wait()


def ends_kernel(wave_ref, mask_ref, ends_ref):
    slices = wave_ref.shape[1]
    lane = iota((BLOCK, LANES), 1)
    ends = jnp.zeros((BLOCK, LANES), F32)
    for f in range(slices):
        for x in range(2):
            place = 4 * (x * slices + f)
            last = pltpu.roll(wave_ref[x, f, :, -LANES:], (place + SHALF) % LANES, 1)
            first = pltpu.roll(wave_ref[x, f, :, :LANES], place + SHALF, 1)
            ends = jnp.where(lane // 2 == place // 2, last, ends)
            ends = jnp.where(lane // 2 == place // 2 + 1, first, ends)
    ends_ref[...] = ends * mask_column(mask_ref)


def rest_kernel(wave_ref, mask_ref, late_ref, link_ref, chip_ref):
    odd = is_odd()
    mask = mask_column(mask_ref)
    slices = wave_ref.shape[1]
    for f in range(slices):
        for x in range(2):
            masked = wave_ref[x, f] * mask
            row = (2 * f + x) * HALO
            chip_ref[row : row + HALO] = at_end(masked, jnp.logical_not(odd))
            if f >= FIRST:
                row -= 2 * FIRST * HALO
                link_ref[row : row + HALO] = at_end(masked, odd)
            elif f >= EARLY:
                row -= 2 * EARLY * HALO
                late_ref[row : row + HALO] = at_end(masked, odd)


def merged_ends(before_ref, after_ref):
    return jnp.where(iota((BLOCK, LANES), 1) % 4 < SHALF, before_ref[...], after_ref[...])


def pack_kernel(before_ref, after_ref, _link_in, link_ref, ends_ref):
    odd = is_odd()
    ends = merged_ends(before_ref, after_ref)
    rows = at_end(ends, odd)
    link_ref[link_ref.shape[0] - HALO // 2 :] = jnp.concatenate([rows[: HALO // 2], rows[HALO // 2 :]], axis=1)
    ends_ref[...] = at_end(ends, jnp.logical_not(odd))


def band_kernel(taper_ref, wave_ref, band_ref, high_ref, low_ref, th_ref, tl_ref, energy_ref):
    shots = wave_ref.shape[3]
    th_ref[...], tl_ref[...] = split(weights_at(taper_ref, iota((shots, shots), 0) - iota((shots, shots), 1)))
    low_half = iota((BLOCK, LANES), 1) < APER
    for f in range(wave_ref.shape[1]):
        at = (f // 2) * LANES
        skewed = []
        for x in range(2):
            taps = jnp.where(low_half == (f % 2 == 0), band_ref[x, :, at : at + LANES], 0.0)
            skewed.append(pltpu.roll(taps, APER * (f % 2), 1, stride=1, stride_axis=0))
        real, imag = skewed
        for row, parts in enumerate([(real, -imag), (imag, real)]):
            for column, part in enumerate(parts):
                place = (f, slice(row * BLOCK, (row + 1) * BLOCK), slice(column * LANES, (column + 1) * LANES))
                high_ref[place], low_ref[place] = split(part)
        squares = wave_ref[0, f] * wave_ref[0, f] + wave_ref[1, f] * wave_ref[1, f]
        squares = jnp.sum(squares, axis=0, keepdims=True)
        energy_ref[f : f + 1, :] = squares[:, :LANES] + squares[:, LANES:]


def framed(frame_ref, own, chip, link, start):
    odd = is_odd()
    left, right = 0, HALO + BLOCK
    frame_ref[HALO : HALO + BLOCK] = own
    frame_ref[pl.ds(pl.multiple_of(jnp.where(odd, left, right), 8), HALO)] = chip
    frame_ref[pl.ds(pl.multiple_of(jnp.where(odd, right, left), 8), HALO)] = link
    return frame_ref[pl.ds(start, LANES)]


def window(frames_ref, wave_ref, mask, chip_ref, link, f, start):
    rows = []
    for x in range(2):
        own = wave_ref[x, f] * mask
        at = (2 * f + x) * HALO
        chip = chip_ref[at : at + HALO]
        other = link(x)
        columns = []
        for tile in range(own.shape[1] // LANES):
            part = slice(tile * LANES, (tile + 1) * LANES)
            columns.append(framed(frames_ref.at[x, tile], own[:, part], chip[:, part], other[:, part], start))
        rows.append(jnp.concatenate(columns, axis=1))
    return jnp.concatenate(rows, axis=0)


def gather_kernel(
    base, shift_ref, wave_ref, mask_ref, high_ref, low_ref, th_ref, tl_ref, link_ref, chip_ref, part_ref, frames_ref,
    ph_ref, pl_ref,
):
    start = SPARE + shift_ref[0]
    mask = mask_column(mask_ref)
    count, rows, shots = part_ref.shape

    def linked(x, i):
        at = (2 * i + x) * HALO
        return link_ref[at : at + HALO]

    for i in range(count):
        f = base + i
        data = window(frames_ref.at[i], wave_ref, mask, chip_ref, lambda x, i=i: linked(x, i), f, start)
        ph_ref[i * rows : (i + 1) * rows], pl_ref[i * rows : (i + 1) * rows] = split(
            product((high_ref[f], low_ref[f]), split(data))
        )
    whole = product((ph_ref[...], pl_ref[...]), (th_ref[...], tl_ref[...]))
    part_ref[...] = whole.reshape(count, rows, shots)


def weights_at(taper_ref, ahead):
    weights = jnp.zeros(ahead.shape, F32)
    for u in range(2 * SHALF + 1):
        weights = jnp.where(ahead == u - SHALF, taper_ref[u], weights)
    return weights


def stored(mult_ref, squares_ref, f, own, extra):
    near = iota(extra.shape, 1) < LANES // 2
    total = jnp.concatenate(
        [own[:, :LANES] + jnp.where(near, extra, 0.0), own[:, LANES:] + jnp.where(near, 0.0, extra)], axis=1
    )
    mult_ref[0, f] = total[:BLOCK]
    mult_ref[1, f] = total[BLOCK:]
    total = jnp.sum(total * total, axis=0, keepdims=True)
    squares_ref[f : f + 1, :] = total[:, :LANES] + total[:, LANES:]


def merge_kernel(
    shift_ref, taper_ref, wave_ref, mask_ref, high_ref, low_ref, th_ref, tl_ref, early_ref, late_ref, chip_ref, ends_ref,
    before_ref, after_ref, mult_ref, edge_ref, squares_ref, kept_ref, frames_ref, ph_ref, pl_ref, part_ref,
):
    start = SPARE + shift_ref[0]
    slices = wave_ref.shape[1]
    shots = wave_ref.shape[3]
    rows = 2 * BLOCK
    count = FIRST - EARLY
    packed = late_ref[late_ref.shape[0] - HALO // 2 :]
    packed = jnp.concatenate([packed[:, :LANES], packed[:, LANES:]], axis=0)
    ends = split(
        framed(frames_ref.at[count, 0, 0], merged_ends(before_ref, after_ref), ends_ref[...], packed, start)
    )
    kind = iota((LANES, LANES), 0) % 4
    source = jnp.where(kind < SHALF, kind - SHALF, kind - SHALF + shots)
    target = iota((LANES, LANES), 1)
    target = jnp.where(target < LANES // 2, target, target + shots - LANES)
    reach = split(weights_at(taper_ref, source - target))
    gather_kernel(
        EARLY, shift_ref, wave_ref, mask_ref, high_ref, low_ref, th_ref, tl_ref, late_ref, chip_ref, part_ref, frames_ref,
        ph_ref, pl_ref,
    )
    kept_ref[...] = wave_ref[:, :KEPT]
    group = 4
    for first in range(0, slices, group):
        shape = (group, rows, LANES)
        owner = iota(shape, 2) // 4 - iota(shape, 0) - first
        edge = jnp.zeros(shape, F32)
        for x in range(2):
            part = slice(x * LANES, (x + 1) * LANES)
            matrices = tuple(ref[first : first + group, :, part].reshape(group * rows, LANES) for ref in (high_ref, low_ref))
            edge = jnp.where(owner == x * slices, product(matrices, ends).reshape(shape), edge)
        edge = product(split(edge.reshape(group * rows, LANES)), reach)
        for f in range(first, first + group):
            extra = edge[(f - first) * rows : (f - first + 1) * rows]
            if f >= FIRST:
                edge_ref[f - FIRST] = extra
            else:
                stored(mult_ref, squares_ref, f, early_ref[f] if f < EARLY else part_ref[f - EARLY], extra)
    squares_ref[FIRST:] = jnp.zeros((slices - FIRST, LANES), F32)


def finish_kernel(
    shift_ref, wave_ref, mask_ref, high_ref, low_ref, th_ref, tl_ref, link_ref, chip_ref, edge_ref, some_ref, data_ref,
    _mult_in, mult_ref, sums_ref, frames_ref, ph_ref, pl_ref, part_ref, squares_ref,
):
    slices = wave_ref.shape[1]
    gather_kernel(
        FIRST, shift_ref, wave_ref, mask_ref, high_ref, low_ref, th_ref, tl_ref, link_ref, chip_ref, part_ref, frames_ref,
        ph_ref, pl_ref,
    )
    squares_ref[...] = some_ref[...]
    for f in range(FIRST, slices):
        stored(mult_ref, squares_ref, f, part_ref[f - FIRST], edge_ref[f - FIRST])
    pred_energy = jnp.sum(squares_ref[...], axis=1, keepdims=True)
    data_energy = jnp.sum(data_ref[...], axis=1, keepdims=True)
    place = iota((slices, LANES), 1) - iota((slices, LANES), 0)
    energies = jnp.where(place == 0, data_energy, jnp.where(place == slices, pred_energy, 0.0))
    sums_ref[...] = jnp.sum(energies, axis=0, keepdims=True)


def subtract_kernel(total_ref, kept_ref, wave_ref, mult_ref, out_ref, held_ref, in_sems, out_sems):
    slices = wave_ref.shape[1]
    reads = {}
    for f in range(KEPT, slices):
        reads[f] = pltpu.make_async_copy(wave_ref.at[:, f], held_ref.at[:, f], in_sems.at[f])
        reads[f].start()
    sums = jnp.sum(total_ref[...], axis=0, keepdims=True)
    row = iota((1, LANES), 1)
    writes = []
    for f in range(slices):
        data = jnp.sum(jnp.where(row == f, sums, 0.0), axis=1, keepdims=True)
        pred = jnp.sum(jnp.where(row == slices + f, sums, 0.0), axis=1, keepdims=True)
        gain = jnp.sqrt((data + 1e-06) / (pred + 1e-06))
        if f in reads:
            reads[f].wait()
        source_ref = held_ref if f in reads else kept_ref
        for x in range(2):
            held_ref[x, f] = source_ref[x, f] - gain * mult_ref[x, f]
        writes.append(pltpu.make_async_copy(held_ref.at[:, f], out_ref.at[:, f], out_sems.at[f]))
        writes[-1].start()
    for copy in writes:
        copy.wait()


VMEM = pl.BlockSpec(memory_space=pltpu.VMEM)
SMEM = pl.BlockSpec(memory_space=pltpu.SMEM)
HBM = pl.BlockSpec(memory_space=pltpu.HBM)
ANY = pl.BlockSpec(memory_space=pl.ANY)


def on_chip(*arrays):
    return [pltpu.with_memory_space_constraint(a, pltpu.VMEM) for a in arrays]


def call(kernel, in_specs, out_shapes, flops, out_specs=None, scratch=(), aliases=None):
    return pl.pallas_call(
        kernel,
        in_specs=in_specs,
        out_specs=out_specs or [VMEM] * len(out_shapes),
        out_shape=out_shapes,
        scratch_shapes=list(scratch),
        input_output_aliases=aliases or {},
        cost_estimate=pl.CostEstimate(flops=flops, transcendentals=0, bytes_accessed=1 << 20),
        compiler_params=pltpu.CompilerParams(vmem_limit_bytes=24 << 20),
    )


def neighbours(axis):
    count = lax.axis_size(axis)
    up = [(i, i + 1) for i in range(count - 1)]
    return up, [(j, i) for i, j in up]


def swaps(axis, first):
    count = lax.axis_size(axis)
    pairs = [(i, i + 1) for i in range(first, count - 1, 2)]
    return pairs + [(j, i) for i, j in pairs]


def per_device(wavefield, surface_band, band_shift, trace_mask, shot_taper):
    _, slices, receivers, shots = wavefield.shape
    src_up, src_down = neighbours(SRC)
    mask = trace_mask.reshape(1, receivers)
    devices = lax.axis_size(SRC_RCV)
    in_hbm = pltpu.with_memory_space_constraint(wavefield, pltpu.HBM)

    rows = 2 * receivers

    def in_vmem(*shape, dtype=F32):
        return pltpu.VMEM(shape, dtype)

    wave, early = call(
        head_kernel,
        [HBM, HBM],
        [in_vmem(2, slices, receivers, shots), in_vmem(2 * EARLY * HALO, shots)],
        1 << 20,
        scratch=[pltpu.VMEM((1, receivers), jnp.int32), pltpu.SemaphoreType.DMA((3,))],
    )(in_hbm, pltpu.with_memory_space_constraint(mask, pltpu.HBM))
    early = lax.ppermute(early, RCV, swaps(RCV, 1))

    wave, band = on_chip(wave, surface_band)
    (ends,) = call(ends_kernel, [VMEM, VMEM], [in_vmem(BLOCK, LANES)], 1 << 20)(wave, mask)
    after = lax.ppermute(ends, SRC, src_down)
    before = lax.ppermute(ends, SRC, src_up)
    late, link, chip = call(
        rest_kernel,
        [VMEM, VMEM],
        [
            in_vmem(2 * (FIRST - EARLY) * HALO + HALO // 2, shots),
            in_vmem(2 * (slices - FIRST) * HALO, shots),
            in_vmem(2 * slices * HALO, shots),
        ],
        1 << 20,
    )(wave, mask)
    chip = lax.ppermute(chip, RCV, swaps(RCV, 0))

    high, low, taper_high, taper_low, data_energy = call(
        band_kernel,
        [SMEM, VMEM, VMEM],
        [
            in_vmem(slices, rows, 2 * LANES, dtype=BF16),
            in_vmem(slices, rows, 2 * LANES, dtype=BF16),
            in_vmem(shots, shots, dtype=BF16),
            in_vmem(shots, shots, dtype=BF16),
            in_vmem(slices, LANES),
        ],
        1 << 28,
    )(shot_taper, wave, band)

    before, after, late = on_chip(before, after, late)
    late, ends = call(
        pack_kernel, [VMEM, VMEM, ANY], [in_vmem(*late.shape), in_vmem(HALO, LANES)], 1 << 16, aliases={2: 0}
    )(before, after, late)
    late = lax.ppermute(late, RCV, swaps(RCV, 1))
    link = lax.ppermute(link, RCV, swaps(RCV, 1))
    ends = lax.ppermute(ends, RCV, swaps(RCV, 0))

    matrices = on_chip(high, low, taper_high, taper_low)
    early, late, link, chip, ends = on_chip(early, late, link, chip, ends)
    frame = (2, shots // LANES, 2 * HALO + BLOCK, LANES)

    def workspace(count, frames):
        return [pltpu.VMEM((frames,) + frame, F32)] + [pltpu.VMEM((count * rows, shots), BF16)] * 2

    (part,) = call(
        functools.partial(gather_kernel, 0),
        [SMEM] + [VMEM] * 8,
        [in_vmem(EARLY, rows, shots)],
        1 << 28,
        scratch=workspace(EARLY, EARLY),
    )(band_shift, wave, mask, *matrices, early, chip)
    middle, last = FIRST - EARLY, slices - FIRST
    multiples, edge, squares, kept = call(
        merge_kernel,
        [SMEM, SMEM] + [VMEM] * 12,
        [
            in_vmem(2, slices, receivers, shots),
            in_vmem(last, rows, LANES),
            in_vmem(slices, LANES),
            in_vmem(2, KEPT, receivers, shots),
        ],
        1 << 28,
        scratch=workspace(middle, middle + 1) + [pltpu.VMEM((middle, rows, shots), F32)],
    )(band_shift, shot_taper, wave, mask, *matrices, *on_chip(part), late, chip, ends, before, after)
    multiples, sums = call(
        finish_kernel,
        [SMEM] + [VMEM] * 11 + [ANY],
        [in_vmem(2, slices, receivers, shots), in_vmem(1, LANES)],
        1 << 28,
        scratch=workspace(last, last) + [pltpu.VMEM((last, rows, shots), F32), pltpu.VMEM((slices, LANES), F32)],
        aliases={12: 0},
    )(band_shift, wave, mask, *matrices, link, chip, *on_chip(edge, squares, data_energy, multiples))

    spread = jnp.broadcast_to(sums[None], (devices, 1, LANES))
    energies = lax.all_to_all(spread, SRC_RCV, 0, 0, tiled=True).reshape(devices, LANES)

    (primaries,) = call(
        subtract_kernel,
        [VMEM, VMEM, HBM, VMEM],
        [jax.ShapeDtypeStruct((2, slices, receivers, shots), F32)],
        1 << 20,
        out_specs=[HBM],
        scratch=[pltpu.VMEM((2, slices, receivers, shots), F32)] + [pltpu.SemaphoreType.DMA((slices,))] * 2,
    )(*on_chip(energies, kept), in_hbm, *on_chip(multiples))
    return (multiples, primaries)


def solution(mesh):
    split_mesh = Mesh(
        mesh.devices.reshape(4, 2, 2, 8, 2), ("src_0", "src_1", "rcv_0", "rcv_1", "rcv_2")
    )
    return jax.shard_map(
        per_device,
        mesh=split_mesh,
        in_specs=(P(None, None, RCV, SRC), P(None, RCV, None), P(RCV), P(RCV), P()),
        out_specs=(P(None, None, RCV, SRC), P(None, None, RCV, SRC)),
        check_vma=False,
    )
```
